32 devices in a mesh: rows: 8 (over z, y), cols: 4 (over x, core).
Axes of the slice: x: 2, y: 2, z: 4, core: 2. Of those that a mesh axis runs over, the one named last changes fastest.
Arguments:
- adjacency_tiles: bfloat16 [192, 12, 128, 128], P(('rows', 'cols')), may hold values from 2.170139e-08 to 0.25
- col_block: int32 [192, 12], P(('rows', 'cols')), may hold values from 0 to 191, as said below
- label_prior: float32 [24576, 256], P(('rows', 'cols')), may hold values from 0.05 to 20.1
- seed_label: int32 [24576], P(('rows', 'cols')), may hold values from 0 to 255
- seed_mask: int32 [24576], P(('rows', 'cols')), may hold values 0 or 1
Outputs:
- labels: float32 [24576, 256], P(('rows', 'cols'))
The draws below stay inside these ranges and needn't reach their ends.
Inputs may be any that keep to these rules, and one draw needn't show every extreme that they name: Row block b is held by device b // 6 of rows+cols, whose rows group is b // (6 * 4). col_block[b, 0] = b. For each device, all its tiles that reference blocks of another rows group reference one and the same block of that group, and each device references every rows group.
All inputs are finite; a program needn't handle non-finite values. No bound on the sum of `seed_mask` on one device may be relied on, other than what follows from the above.
Results may differ from the reference program's by a relative error of at most 0.00041.
Values may be sent and summed in bfloat16 or wider, within the bound.
A program may use at most 64 MiB of HBM per device.

```python
import jax
import jax.numpy as jnp
from jax import lax

CLASSES = 256
BLOCK = 128
DEGREE = 12
HOPS = 4
BLOCKS_DEV = 6
BLOCKS = 192
NODES = 24576
N_ROWS = 8
N_COLS = 4


def draw_col_block(key, part):
    device_count = BLOCKS // BLOCKS_DEV
    group_size = N_COLS * BLOCKS_DEV
    slot_count = BLOCKS_DEV * (DEGREE - 1)

    def per_device(device):
        device_key = jax.random.fold_in(jax.random.fold_in(key, 7177), device)
        k_within, k_group, k_local, k_coin, k_perm = jax.random.split(device_key, 5)
        home_group = device // N_COLS
        chosen = jax.random.randint(k_within, (N_ROWS,), 0, group_size)
        extra_group = jax.random.randint(k_group, (slot_count - N_ROWS,), 0, N_ROWS)
        coin_flip = jax.random.randint(k_coin, (slot_count - N_ROWS,), 0, 2)
        extra_group = jnp.where(coin_flip == 0, home_group, extra_group)
        groups_all = jnp.concatenate([jnp.arange(N_ROWS, dtype=jnp.int32), extra_group.astype(jnp.int32)])
        local_pick = jax.random.randint(k_local, (slot_count,), 0, group_size)
        within_all = jnp.where(groups_all == home_group, local_pick, chosen[groups_all])
        shuffle = jax.random.permutation(k_perm, slot_count)
        picked = (groups_all * group_size + within_all)[shuffle].reshape(BLOCKS_DEV, DEGREE - 1)
        diagonal = device * BLOCKS_DEV + jnp.arange(BLOCKS_DEV, dtype=jnp.int32)
        return jnp.concatenate([diagonal[:, None], picked.astype(jnp.int32)], axis=1)
    result = jax.vmap(per_device)(jnp.arange(device_count, dtype=jnp.int32))
    return result.reshape(BLOCKS, DEGREE).astype(jnp.int32)


def draw_adjacency_tiles(key, part):
    k_scale, k_entry, k_pick = jax.random.split(jax.random.fold_in(key, 3301), 3)
    span = jnp.log(jnp.float32(100.0))
    tile_scale = jnp.exp(span * jax.random.uniform(k_scale, (BLOCKS, DEGREE), jnp.float32))
    tile_scale = tile_scale / jnp.sum(tile_scale, axis=1, keepdims=True)
    shape = (BLOCKS, DEGREE, BLOCK, BLOCK)
    entries = jnp.exp(jax.random.uniform(k_entry, shape, jnp.float32, jnp.log(0.5), jnp.log(2.0)))
    dominant = jax.random.randint(k_pick, shape, 0, 16) == 0
    pattern = jnp.where(dominant, entries * (16.0 / BLOCK), jnp.float32(0.01 / BLOCK))
    values = tile_scale[:, :, None, None] * pattern
    return values.astype(jnp.bfloat16)


def draw_label_prior(key, part):
    k_base, k_pick, k_boost = jax.random.split(jax.random.fold_in(key, 5407), 3)
    base = jnp.exp(jax.random.uniform(k_base, (NODES, CLASSES), jnp.float32, jnp.log(0.05), 0.0))
    picked = jax.random.randint(k_pick, (NODES, CLASSES), 0, 16) == 0
    boost = jnp.exp(3.0 * jax.random.uniform(k_boost, (NODES, CLASSES), jnp.float32))
    factor = jnp.where(picked, boost, jnp.float32(1.0))
    return (base * factor).astype(jnp.float32)


def with_ends(values, rng, low, high):
    spot = [jax.random.randint(jax.random.fold_in(rng, axis), (), 0, length) for axis, length in enumerate(values.shape)]
    main_axis = values.shape.index(max(values.shape))
    beside = spot[:main_axis] + [(spot[main_axis] + 1) % values.shape[main_axis]] + spot[main_axis + 1:]
    return values.at[tuple(spot)].set(low).at[tuple(beside)].set(high)


def setup_inputs(seed: int = 0) -> dict:
    seeds = jax.random.split(jax.random.key(seed), 6)
    adjacency_tiles = draw_adjacency_tiles(jax.random.fold_in(seeds[5], 71), 0)
    col_block = draw_col_block(jax.random.fold_in(seeds[5], 71), 0)
    label_prior = draw_label_prior(jax.random.fold_in(seeds[5], 71), 0)
    seed_label = with_ends(jax.random.randint(seeds[3], (NODES,), 0, CLASSES), jax.random.fold_in(seeds[3], 1), 0, CLASSES - 1).astype(jnp.int32)
    seed_mask = with_ends((jax.random.randint(seeds[4], (NODES,), 0, 4) < 1).astype(jnp.int32), jax.random.fold_in(seeds[4], 1), 0, 1)
    return {"adjacency_tiles": adjacency_tiles, "col_block": col_block, "label_prior": label_prior, "seed_label": seed_label, "seed_mask": seed_mask}


ALPHA = 0.85
SEED_BOOST = 8.0


def prepare(label_prior, seed_label, seed_mask):
    classes = label_prior.shape[1]
    one_hot = (seed_label[:, None] == jnp.arange(classes, dtype=jnp.int32)[None, :]).astype(jnp.float32)
    anchor_raw = label_prior + SEED_BOOST * seed_mask[:, None].astype(jnp.float32) * one_hot
    return anchor_raw * (classes / jnp.sum(anchor_raw, axis=1, keepdims=True))


def reference(adjacency_tiles, col_block, label_prior, seed_label, seed_mask):
    anchor = prepare(label_prior, seed_label, seed_mask)
    labels = anchor
    for hop_index in range(HOPS):
        sent_blocks = labels.astype(jnp.bfloat16).reshape(BLOCKS, BLOCK, CLASSES)

        def per_block(pair_in):
            tile_set, col_ids = pair_in
            operand = sent_blocks[col_ids]
            return jnp.einsum("kij,kjc->ic", tile_set.astype(jnp.float32), operand.astype(jnp.float32))

        spread = lax.map(per_block, (adjacency_tiles, col_block), batch_size=16).reshape(NODES, CLASSES)
        blended = ALPHA * spread + (1.0 - ALPHA) * anchor
        labels = blended * (CLASSES / jnp.sum(blended, axis=1, keepdims=True))
    return labels
```

```python
import functools

import jax
import jax.numpy as jnp
from jax import lax
from jax.experimental import pallas as pl
from jax.experimental.pallas import tpu as pltpu
from jax.sharding import PartitionSpec as P

HOPS = 4
STREAMS = 2
CHUNK_PARTS = (1, 1, 2, 4)
CHUNKS = len(CHUNK_PARTS)
ALPHA = 0.85
SEED_BOOST = 8.0
LANES = 128
VMEM_LIMIT = 67_043_328
SPARE = 64 * 1024
MESH = pl.DeviceIdType.MESH


def kernel(
    n_rows, n_cols, blocks_dev, degree, block_rows, classes,
    col_block_hbm, prior_hbm, label_hbm, mask_hbm, adj_hbm, out_ref,
    tables, remote, reply, sums, sums_remote, sums_reply, sums_part, scale_ref,
    adj, anchor_ref, index_ref, wanted_ref, asked_v, asked_s,
    col_block_ref, prior_ref, label_ref, mask_ref, in_sem,
    adj_sem, asked_send, asked_recv, asked_copy,
    near_send, near_recv, far_send, far_recv, fwd_send, fwd_recv, rep_send, rep_recv,
    sums_send, sums_recv, srep_send, srep_recv,
):
    row = lax.axis_index("rows")
    col = lax.axis_index("cols")
    group = n_cols * blocks_dev
    lanes = classes // STREAMS
    width = 2 if n_cols % 2 == 0 else 1
    pairs = n_cols // width
    pair, low = col // width, col % width
    mate = pair * width + (width - 1 - low)
    unit = block_rows // sum(CHUNK_PARTS)
    starts = [unit * sum(CHUNK_PARTS[:q]) for q in range(CHUNKS)]
    sizes = [unit * part for part in CHUNK_PARTS]
    peers = n_rows - 1

    def far_col(j):
        return ((pair + j) % pairs) * width + low

    def from_col(j):
        return ((pair + pairs - j) % pairs) * width + low

    def each_peer(body):
        half = n_rows // 2
        def step(i):
            if isinstance(i, int):
                d = half + ((i + 1) // 2) * (1 - 2 * (i % 2))
            else:
                d = half + lax.div(i + 1, 2) * (1 - 2 * lax.rem(i, 2))
            body((row + d + n_rows) % n_rows)
        if n_rows <= 8:
            for i in range(peers):
                step(i)
        else:
            def loop(i, carry):
                step(i)
                return carry
            lax.fori_loop(0, peers, loop, 0)

    adj_copy = pltpu.make_async_copy(adj_hbm, adj, adj_sem)
    loads = [
        pltpu.make_async_copy(source, target, in_sem.at[i])
        for i, (source, target) in enumerate([
            (label_hbm, label_ref),
            (mask_hbm, mask_ref),
            (prior_hbm, prior_ref),
            (col_block_hbm, col_block_ref),
        ])
    ]
    for load in loads:
        load.start()
    adj_copy.start()

    barrier = pltpu.get_barrier_semaphore()
    for j in range(1, n_cols):
        pl.semaphore_signal(
            barrier, inc=1, device_id=(row, (col + j) % n_cols), device_id_type=MESH
        )
    each_peer(
        lambda other: pl.semaphore_signal(
            barrier, inc=1, device_id=(other, col), device_id_type=MESH
        )
    )

    ones = jnp.ones((8, lanes), jnp.bfloat16)

    def keep(p, s, b, labels):
        sent = labels.astype(jnp.bfloat16)
        for q in range(CHUNKS):
            tables[p][s][q][col * blocks_dev + b] = sent[starts[q] : starts[q] + sizes[q], :]
        total = lax.dot_general(
            ones, sent, (((1,), (1,)), ((), ())), preferred_element_type=jnp.float32
        )[:1, :]
        if s > 0:
            total = total + sums_part[b]
        if s < STREAMS - 1:
            sums_part[b] = total
        else:
            sums[p][col * blocks_dev + b] = total

    for load in loads:
        load.wait()
    code = jnp.where(mask_ref[...] > 0, label_ref[...], -1)
    for b in range(blocks_dev):
        here = slice(b * block_rows, (b + 1) * block_rows)
        across = jnp.broadcast_to(code[b : b + 1, :], (block_rows, block_rows)).T
        class_id = lax.broadcasted_iota(jnp.int32, (block_rows, classes), 1)
        across = jnp.concatenate([across] * (classes // block_rows), axis=1)
        raw = prior_ref[here, :] + jnp.where(class_id == across, SEED_BOOST, 0.0)
        anchor = raw * (classes / jnp.sum(raw, axis=1, keepdims=True))
        anchor_ref[here, :] = anchor
        for s in range(STREAMS):
            keep(0, s, b, anchor[:, s * lanes : (s + 1) * lanes])

    lane = lax.broadcasted_iota(jnp.int32, wanted_ref.shape, 1)
    wanted = jnp.zeros(wanted_ref.shape, jnp.int32)
    for b in range(blocks_dev):
        for k in range(degree):
            block = col_block_ref[b, k]
            owner = lax.div(block, group)
            within = block - owner * group
            index_ref[b * degree + k] = jnp.where(owner == row, within, group + owner)
            wanted = jnp.where(lane == owner, within, wanted)
    wanted_ref[...] = wanted

    pl.semaphore_wait(barrier, n_cols - 1 + peers)

    def send_wanted(other):
        pltpu.make_async_remote_copy(
            src_ref=wanted_ref, dst_ref=asked_v.at[row], send_sem=asked_send, recv_sem=asked_recv,
            device_id=(other, col), device_id_type=MESH,
        ).start()

    each_peer(send_wanted)

    def part(p, s, owner, q):
        return tables[p][s][q].at[pl.ds(owner * blocks_dev, blocks_dev)]

    def near(p, s, q):
        ref = part(p, s, col, q)
        return pltpu.make_async_remote_copy(
            src_ref=ref, dst_ref=ref,
            send_sem=near_send.at[p, s, q], recv_sem=near_recv.at[p, s, q],
            device_id=(row, mate), device_id_type=MESH,
        )

    def far(p, s, j, q):
        ref = part(p, s, col, q)
        return pltpu.make_async_remote_copy(
            src_ref=ref, dst_ref=ref,
            send_sem=far_send.at[p, s, j - 1, q], recv_sem=far_recv.at[p, s, j - 1, q],
            device_id=(row, far_col(j)), device_id_type=MESH,
        )

    def forward(p, s, j, q):
        ref = part(p, s, from_col(j), q)
        return pltpu.make_async_remote_copy(
            src_ref=ref, dst_ref=ref,
            send_sem=fwd_send.at[p, s, j - 1, q], recv_sem=fwd_recv.at[p, s, j - 1, q],
            device_id=(row, mate), device_id_type=MESH,
        )

    def sums_to(p, j):
        ref = sums[p].at[pl.ds(col * blocks_dev, blocks_dev)]
        return pltpu.make_async_remote_copy(
            src_ref=ref, dst_ref=ref,
            send_sem=sums_send.at[p, j - 1], recv_sem=sums_recv.at[p, j - 1],
            device_id=(row, (col + j) % n_cols), device_id_type=MESH,
        )

    def start_sums(p):
        for j in range(1, n_cols):
            sums_to(p, j).start()

    def start_gather(p, s):
        for q in range(CHUNKS):
            for j in range(1, pairs):
                far(p, s, j, q).start()
            if width == 2:
                near(p, s, q).start()

    def relay_sums(p):
        for j in range(1, n_cols):
            sums_to(p, j).wait_recv()

        def answer(other):
            sums_reply[other] = sums[p][asked_s[other, 0, row]]
            pltpu.make_async_remote_copy(
                src_ref=sums_reply.at[other], dst_ref=sums_remote.at[p, row],
                send_sem=srep_send.at[p], recv_sem=srep_recv.at[p],
                device_id=(other, col), device_id_type=MESH,
            ).start()

        each_peer(answer)

    def relay(p, s):
        for q in range(CHUNKS):
            rows_q = pl.ds(starts[q], sizes[q])
            for j in range(1, pairs):
                far(p, s, j, q).wait_recv()
                if width == 2:
                    forward(p, s, j, q).start()
            if width == 2:
                near(p, s, q).wait_recv()
                for j in range(1, pairs):
                    forward(p, s, j, q).wait_recv()

            def answer(other):
                reply[s, other, rows_q, :] = tables[p][s][q][asked_s[other, 0, row]]
                pltpu.make_async_remote_copy(
                    src_ref=reply.at[s, other, rows_q, :],
                    dst_ref=remote.at[p, s, row, rows_q, :],
                    send_sem=rep_send.at[p, s], recv_sem=rep_recv.at[p, s],
                    device_id=(other, col), device_id_type=MESH,
                ).start()

            each_peer(answer)

    def operand(p, s, b, k):
        index = index_ref[b * degree + k]
        return [tables[p][s][q][index] for q in range(CHUNKS)]

    def row_scale(p, b):
        here = slice(b * block_rows, (b + 1) * block_rows)
        total = jnp.zeros((block_rows, block_rows), jnp.float32)
        for k in range(degree):
            total = total + adj[b, k].astype(jnp.float32) * sums[p][index_ref[b * degree + k]]
        rest = anchor_ref[here, :block_rows]
        for i in range(1, classes // block_rows):
            rest = rest + anchor_ref[here, i * block_rows : (i + 1) * block_rows]
        total = ALPHA * total + (1.0 - ALPHA) * rest
        return classes / jnp.sum(total, axis=1, keepdims=True)

    def finish(h, s):
        p, last = h % 2, h == HOPS - 1
        got = remote.at[p, s, pl.ds(0, peers)]
        pltpu.make_async_copy(got, got, rep_recv.at[p, s]).wait()
        if s == 0:
            got = sums_remote.at[p, pl.ds(0, peers)]
            pltpu.make_async_copy(got, got, srep_recv.at[p]).wait()

        def fold(other):
            for q in range(CHUNKS):
                tables[p][s][q][group + other] = remote[p, s, other, pl.ds(starts[q], sizes[q]), :]
            if s == 0:
                sums[p][group + other] = sums_remote[p, other]

        each_peer(fold)

        step = 2 if degree % 2 == 0 else 1
        mine = slice(s * lanes, (s + 1) * lanes)
        for b in range(blocks_dev):
            here = slice(b * block_rows, (b + 1) * block_rows)
            spread = jnp.zeros((block_rows, lanes), jnp.float32)
            for k in range(0, degree, step):
                lhs = jnp.concatenate([adj[b, k + i] for i in range(step)], axis=1)
                rhs = jnp.concatenate(sum([operand(p, s, b, k + i) for i in range(step)], []), axis=0)
                spread = spread + jnp.dot(lhs, rhs, preferred_element_type=jnp.float32)
            if s == 0:
                scale = jnp.broadcast_to(row_scale(p, b), (block_rows, lanes))
                scale_ref[here, :] = scale
            else:
                scale = scale_ref[here, :]
            labels = (ALPHA * spread + (1.0 - ALPHA) * anchor_ref[here, mine]) * scale
            if last:
                out_ref[here, mine] = labels
            else:
                keep(1 - p, s, b, labels)

        for q in range(CHUNKS):
            for j in range(1, pairs):
                far(p, s, j, q).wait_send()
                if width == 2:
                    forward(p, s, j, q).wait_send()
            if width == 2:
                near(p, s, q).wait_send()
        sent = reply.at[s, pl.ds(0, peers)]
        pltpu.make_async_copy(sent, sent, rep_send.at[p, s]).wait()
        if s == STREAMS - 1:
            for j in range(1, n_cols):
                sums_to(p, j).wait_send()
            sent = sums_reply.at[pl.ds(0, peers)]
            pltpu.make_async_copy(sent, sent, srep_send.at[p]).wait()

        if not last:
            if s == STREAMS - 1:
                start_sums(1 - p)
            start_gather(1 - p, s)

    start_sums(0)
    for s in range(STREAMS):
        start_gather(0, s)

    all_asked = asked_v.at[pl.ds(0, peers)]
    pltpu.make_async_copy(all_asked, all_asked, asked_recv).wait()
    pltpu.make_async_copy(all_asked, all_asked, asked_send).wait()
    to_scalar = pltpu.make_async_copy(asked_v, asked_s, asked_copy)
    to_scalar.start()
    to_scalar.wait()

    relay_sums(0)
    for s in range(STREAMS):
        relay(0, s)
    adj_copy.wait()

    for h in range(HOPS):
        for s in range(STREAMS):
            finish(h, s)
            if h < HOPS - 1:
                if s == STREAMS - 1:
                    relay_sums((h + 1) % 2)
                relay((h + 1) % 2, s)


def local(adjacency_tiles, col_block, label_prior, seed_label, seed_mask):
    blocks_dev, degree, block_rows, _ = adjacency_tiles.shape
    nodes, classes = label_prior.shape
    n_rows = lax.axis_size("rows")
    n_cols = lax.axis_size("cols")
    group = n_cols * blocks_dev
    lanes = classes // STREAMS
    padded = -(-n_rows // LANES) * LANES
    pairs = max(n_cols // 2 if n_cols % 2 == 0 else n_cols, 2)
    others = max(n_cols - 1, 1)
    unit = block_rows // sum(CHUNK_PARTS)
    dma = pltpu.SemaphoreType.DMA
    vmem = pl.BlockSpec(memory_space=pltpu.VMEM)
    return pl.pallas_call(
        functools.partial(kernel, n_rows, n_cols, blocks_dev, degree, block_rows, classes),
        out_shape=jax.ShapeDtypeStruct((nodes, classes), jnp.float32),
        in_specs=[
            pl.BlockSpec(memory_space=pl.ANY),
        ] * 5,
        out_specs=vmem,
        scratch_shapes=[
            [
                [
                    [
                        pltpu.VMEM((group + n_rows, unit * part, lanes), jnp.bfloat16)
                        for part in CHUNK_PARTS
                    ]
                    for _ in range(STREAMS)
                ]
                for _ in range(2)
            ],
            pltpu.VMEM((2, STREAMS, n_rows, block_rows, lanes), jnp.bfloat16),
            pltpu.VMEM((STREAMS, n_rows, block_rows, lanes), jnp.bfloat16),
            [pltpu.VMEM((group + n_rows, 1, block_rows), jnp.float32) for _ in range(2)],
            pltpu.VMEM((2, n_rows, 1, block_rows), jnp.float32),
            pltpu.VMEM((n_rows, 1, block_rows), jnp.float32),
            pltpu.VMEM((blocks_dev, 1, block_rows), jnp.float32),
            pltpu.VMEM((nodes, lanes), jnp.float32),
            pltpu.VMEM(adjacency_tiles.shape, jnp.bfloat16),
            pltpu.VMEM((nodes, classes), jnp.float32),
            pltpu.SMEM((blocks_dev * degree,), jnp.int32),
            pltpu.VMEM((1, padded), jnp.int32),
            pltpu.VMEM((n_rows, 1, padded), jnp.int32),
            pltpu.SMEM((n_rows, 1, padded), jnp.int32),
            pltpu.SMEM(col_block.shape, jnp.int32),
            pltpu.VMEM((nodes, classes), jnp.float32),
            pltpu.VMEM((blocks_dev, block_rows), jnp.int32),
            pltpu.VMEM((blocks_dev, block_rows), jnp.int32),
            dma((4,)),
            dma, dma, dma, dma,
            dma((2, STREAMS, CHUNKS)), dma((2, STREAMS, CHUNKS)),
            dma((2, STREAMS, pairs - 1, CHUNKS)), dma((2, STREAMS, pairs - 1, CHUNKS)),
            dma((2, STREAMS, pairs - 1, CHUNKS)), dma((2, STREAMS, pairs - 1, CHUNKS)),
            dma((2, STREAMS)), dma((2, STREAMS)),
            dma((2, others)), dma((2, others)),
            dma((2,)), dma((2,)),
        ],
        compiler_params=pltpu.CompilerParams(
            collective_id=0, has_side_effects=True, vmem_limit_bytes=VMEM_LIMIT - 4 * nodes * classes - SPARE
        ),
    )(
        col_block,
        label_prior,
        seed_label.reshape(blocks_dev, block_rows),
        seed_mask.reshape(blocks_dev, block_rows),
        adjacency_tiles,
    )


def solution(mesh):
    in_specs = (
        P(("rows", "cols"), None, None, None),
        P(("rows", "cols"), None),
        P(("rows", "cols"), None),
        P(("rows", "cols")),
        P(("rows", "cols")),
    )
    out_specs = P(("rows", "cols"), None)
    return jax.shard_map(local, mesh=mesh, in_specs=in_specs, out_specs=out_specs, check_vma=False)
```

```python
import functools

import jax
import jax.numpy as jnp
from jax import lax
from jax.experimental import pallas as pl
from jax.experimental.pallas import tpu as pltpu
from jax.sharding import PartitionSpec as P

HOPS = 4
STREAMS = 2
CHUNK_PARTS = (2, 2, 4)
HEAD = "S G0 G1 G2".split()
EARLY = "U A0 A1".split()
LATE = "A2".split()
CHUNKS = len(CHUNK_PARTS)
ALPHA = 0.85
SEED_BOOST = 8.0
LANES = 128
VMEM_LIMIT = 67_043_328
SPARE = 64 * 1024
MESH = pl.DeviceIdType.MESH


def kernel(
    n_rows, n_cols, blocks_dev, degree, block_rows, classes,
    col_block_hbm, prior_hbm, label_hbm, mask_hbm, adj_hbm, out_ref,
    tables, remote, reply, landed, sums, sums_remote, sums_reply, sums_part, scale_ref, blend_ref,
    adj, anchor_ref, index_ref, wanted_ref, asked_v, asked_s,
    col_block_ref, prior_ref, label_ref, mask_ref, in_sem,
    adj_sem, asked_send, asked_recv, asked_copy,
    near_send, near_recv, far_send, far_recv, fwd_send, fwd_recv, rep_send, rep_recv,
    sums_send, sums_recv, srep_send, srep_recv,
):
    row = lax.axis_index("rows")
    col = lax.axis_index("cols")
    group = n_cols * blocks_dev
    lanes = classes // STREAMS
    pairs = n_cols // 2
    pair, low = col // 2, col % 2
    mate = pair * 2 + 1 - low
    unit = block_rows // sum(CHUNK_PARTS)
    starts = [unit * sum(CHUNK_PARTS[:q]) for q in range(CHUNKS)]
    sizes = [unit * part for part in CHUNK_PARTS]
    halves = [size // 2 for size in sizes]
    peers = n_rows - 1

    def each_peer(body):
        half = n_rows // 2
        def step(i):
            if isinstance(i, int):
                d = half + ((i + 1) // 2) * (1 - 2 * (i % 2))
            else:
                d = half + lax.div(i + 1, 2) * (1 - 2 * lax.rem(i, 2))
            body((row + d + n_rows) % n_rows)
        if n_rows <= 8:
            for i in range(peers):
                step(i)
        else:
            def loop(i, carry):
                step(i)
                return carry
            lax.fori_loop(0, peers, loop, 0)

    adj_copy = pltpu.make_async_copy(adj_hbm, adj, adj_sem)
    loads = [
        pltpu.make_async_copy(source, target, in_sem.at[i])
        for i, (source, target) in enumerate([
            (col_block_hbm, col_block_ref),
            (label_hbm, label_ref),
            (mask_hbm, mask_ref),
            (prior_hbm, prior_ref),
        ])
    ]
    for load in loads:
        load.start()
    adj_copy.start()

    barrier = pltpu.get_barrier_semaphore()
    for j in range(1, n_cols):
        pl.semaphore_signal(
            barrier, inc=1, device_id=(row, (col + j) % n_cols), device_id_type=MESH
        )
    def greet(other):
        for r in range(2):
            pl.semaphore_signal(
                barrier, inc=1, device_id=(other, pair * 2 + r), device_id_type=MESH
            )

    each_peer(greet)

    ones = jnp.ones((8, lanes), jnp.bfloat16)

    def keep(p, s, b, labels):
        sent = labels.astype(jnp.bfloat16)
        for q in range(CHUNKS):
            tables[p][s][q][col * blocks_dev + b] = sent[starts[q] : starts[q] + sizes[q], :]

    def sum_rows(p, s):
        for b in range(blocks_dev):
            mine = col * blocks_dev + b
            sent = jnp.concatenate([tables[p][s][q][mine] for q in range(CHUNKS)], axis=0)
            total = lax.dot_general(
                ones, sent, (((1,), (1,)), ((), ())), preferred_element_type=jnp.float32
            )[:1, :]
            if s > 0:
                total = total + sums_part[b]
            if s < STREAMS - 1:
                sums_part[b] = total
            else:
                sums[p][mine] = total

    loads[0].wait()
    lane = lax.broadcasted_iota(jnp.int32, wanted_ref.shape, 1)
    wanted = jnp.zeros(wanted_ref.shape, jnp.int32)
    for b in range(blocks_dev):
        for k in range(degree):
            block = col_block_ref[b, k]
            owner = lax.div(block, group)
            within = block - owner * group
            index_ref[b * degree + k] = jnp.where(owner == row, within, group + owner)
            wanted = jnp.where(lane == owner, within, wanted)
    wanted_ref[...] = wanted

    pl.semaphore_wait(barrier, n_cols - 1 + 2 * peers)

    def send_wanted(other):
        for r in range(2):
            pltpu.make_async_remote_copy(
                src_ref=wanted_ref, dst_ref=asked_v.at[low, row],
                send_sem=asked_send, recv_sem=asked_recv,
                device_id=(other, pair * 2 + r), device_id_type=MESH,
            ).start()

    each_peer(send_wanted)

    for load in loads[1:]:
        load.wait()
    code = jnp.where(mask_ref[...] > 0, label_ref[...], -1)
    for b in range(blocks_dev):
        here = slice(b * block_rows, (b + 1) * block_rows)
        across = jnp.broadcast_to(code[b : b + 1, :], (block_rows, block_rows)).T
        class_id = lax.broadcasted_iota(jnp.int32, (block_rows, classes), 1)
        across = jnp.concatenate([across] * (classes // block_rows), axis=1)
        raw = prior_ref[here, :] + jnp.where(class_id == across, SEED_BOOST, 0.0)
        anchor = raw * (classes / jnp.sum(raw, axis=1, keepdims=True))
        anchor_ref[here, :] = anchor
        for s in range(STREAMS):
            keep(0, s, b, anchor[:, s * lanes : (s + 1) * lanes])

    def rows_of(q, r):
        return pl.ds(pl.multiple_of(r * halves[q], 16), halves[q])

    def near(p, s, q):
        ref = tables[p][s][q].at[pl.ds(col * blocks_dev, blocks_dev)]
        return pltpu.make_async_remote_copy(
            src_ref=ref, dst_ref=ref,
            send_sem=near_send.at[p, s, q], recv_sem=near_recv.at[p, s, q],
            device_id=(row, mate), device_id_type=MESH,
        )

    def far(p, s, j, q, d):
        r = (low + d) % 2
        ref = tables[p][s][q].at[pl.ds(col * blocks_dev, blocks_dev), rows_of(q, r), :]
        return pltpu.make_async_remote_copy(
            src_ref=ref, dst_ref=ref,
            send_sem=far_send.at[p, s, j - 1, q, d], recv_sem=far_recv.at[p, s, j - 1, q, d],
            device_id=(row, ((pair + j) % pairs) * 2 + r), device_id_type=MESH,
        )

    def forward(p, s, j, q):
        first = ((pair + pairs - j) % pairs) * 2 * blocks_dev
        return pltpu.make_async_remote_copy(
            src_ref=tables[p][s][q].at[pl.ds(first, 2 * blocks_dev), rows_of(q, low), :],
            dst_ref=landed[p][s][q].at[pl.ds((j - 1) * 2 * blocks_dev, 2 * blocks_dev)],
            send_sem=fwd_send.at[p, s, j - 1, q], recv_sem=fwd_recv.at[p, s, j - 1, q],
            device_id=(row, mate), device_id_type=MESH,
        )

    def sums_to(p, j):
        ref = sums[p].at[pl.ds(col * blocks_dev, blocks_dev)]
        return pltpu.make_async_remote_copy(
            src_ref=ref, dst_ref=ref,
            send_sem=sums_send.at[p, j - 1], recv_sem=sums_recv.at[p, j - 1],
            device_id=(row, (col + j) % n_cols), device_id_type=MESH,
        )

    def start_sums(p):
        for j in range(1, n_cols):
            sums_to(p, j).start()

    def start_gather(p, s, q):
        for j in range(1, pairs):
            for d in range(2):
                far(p, s, j, q, d).start()
        near(p, s, q).start()

    def relay_sums(p):
        for j in range(1, n_cols):
            sums_to(p, j).wait_recv()

        def answer(other):
            sums_reply[other] = sums[p][asked_s[low, other, 0, row]]
            pltpu.make_async_remote_copy(
                src_ref=sums_reply.at[other], dst_ref=sums_remote.at[p, row],
                send_sem=srep_send.at[p], recv_sem=srep_recv.at[p],
                device_id=(other, col), device_id_type=MESH,
            ).start()

        each_peer(answer)

    def relay(p, s, steps):
        for kind, q in [(text[0], int(text[1:] or 0)) for text in steps]:
            if kind == "G":
                start_gather(p, s, q)
                continue
            if kind == "S":
                sum_rows(p, s)
                if s == STREAMS - 1:
                    start_sums(p)
                continue
            if kind == "U":
                if s == STREAMS - 1:
                    relay_sums(p)
                continue
            for j in range(1, pairs):
                for d in range(2):
                    far(p, s, j, q, d).wait_recv()
            near(p, s, q).wait_recv()
            rows_q = pl.ds(pl.multiple_of(starts[q] + low * halves[q], 16), halves[q])

            def answer(other):
                for r in range(2):
                    reply[s, r, other, rows_q, :] = tables[p][s][q][
                        asked_s[r, other, 0, row], rows_of(q, low), :
                    ]
                    pltpu.make_async_remote_copy(
                        src_ref=reply.at[s, r, other, rows_q, :],
                        dst_ref=remote.at[p, s, row, rows_q, :],
                        send_sem=rep_send.at[p, s], recv_sem=rep_recv.at[p, s],
                        device_id=(other, pair * 2 + r), device_id_type=MESH,
                    ).start()

            each_peer(answer)
            for j in range(1, pairs):
                forward(p, s, j, q).start()

    def operand(p, s, b, k):
        index = index_ref[b * degree + k]
        return [tables[p][s][q][index] for q in range(CHUNKS)]

    def row_scale(p, b):
        here = slice(b * block_rows, (b + 1) * block_rows)
        total = jnp.zeros((block_rows, block_rows), jnp.float32)
        for k in range(degree):
            total = total + adj[b, k].astype(jnp.float32) * sums[p][index_ref[b * degree + k]]
        rest = anchor_ref[here, :block_rows]
        for i in range(1, classes // block_rows):
            rest = rest + anchor_ref[here, i * block_rows : (i + 1) * block_rows]
        total = ALPHA * total + (1.0 - ALPHA) * rest
        return classes / jnp.sum(total, axis=1, keepdims=True)

    def finish(h, s):
        p, last = h % 2, h == HOPS - 1
        got = remote.at[p, s, pl.ds(0, peers)]
        pltpu.make_async_copy(got, got, rep_recv.at[p, s]).wait()

        for q in range(CHUNKS):
            for j in range(1, pairs):
                forward(p, s, j, q).wait_recv()
                first = ((pair + pairs - j) % pairs) * 2 * blocks_dev
                tables[p][s][q][pl.ds(first, 2 * blocks_dev), rows_of(q, 1 - low), :] = landed[p][s][q][
                    pl.ds((j - 1) * 2 * blocks_dev, 2 * blocks_dev)
                ]

        def fold(other):
            for q in range(CHUNKS):
                tables[p][s][q][group + other] = remote[p, s, other, pl.ds(starts[q], sizes[q]), :]

        each_peer(fold)

        step = 2 if degree % 2 == 0 else 1
        mine = slice(s * lanes, (s + 1) * lanes)

        def blend(b):
            here = slice(b * block_rows, (b + 1) * block_rows)
            spread = jnp.zeros((block_rows, lanes), jnp.float32)
            for k in range(0, degree, step):
                lhs = jnp.concatenate([adj[b, k + i] for i in range(step)], axis=1)
                rhs = jnp.concatenate(sum([operand(p, s, b, k + i) for i in range(step)], []), axis=0)
                spread = spread + jnp.dot(lhs, rhs, preferred_element_type=jnp.float32)
            return ALPHA * spread + (1.0 - ALPHA) * anchor_ref[here, mine]

        if s == 0:
            for b in range(blocks_dev):
                blend_ref[b * block_rows : (b + 1) * block_rows, :] = blend(b)
            got = sums_remote.at[p, pl.ds(0, peers)]
            pltpu.make_async_copy(got, got, srep_recv.at[p]).wait()

            def fold_sums(other):
                sums[p][group + other] = sums_remote[p, other]

            each_peer(fold_sums)

        for b in range(blocks_dev):
            here = slice(b * block_rows, (b + 1) * block_rows)
            if s == 0:
                scale = jnp.broadcast_to(row_scale(p, b), (block_rows, lanes))
                scale_ref[here, :] = scale
                labels = blend_ref[here, :] * scale
            else:
                labels = blend(b) * scale_ref[here, :]
            if last:
                out_ref[here, mine] = labels
            else:
                keep(1 - p, s, b, labels)

        for q in range(CHUNKS):
            for j in range(1, pairs):
                for d in range(2):
                    far(p, s, j, q, d).wait_send()
                forward(p, s, j, q).wait_send()
            near(p, s, q).wait_send()
        for r in range(2):
            sent = reply.at[s, r, pl.ds(0, peers), pl.ds(0, block_rows // 2), :]
            pltpu.make_async_copy(sent, sent, rep_send.at[p, s]).wait()
        if s == STREAMS - 1:
            for j in range(1, n_cols):
                sums_to(p, j).wait_send()
            sent = sums_reply.at[pl.ds(0, peers)]
            pltpu.make_async_copy(sent, sent, srep_send.at[p]).wait()


    for s in range(STREAMS):
        relay(0, s, ["S"])
    for s in range(STREAMS):
        relay(0, s, HEAD[1:])

    all_asked = asked_v.at[:, pl.ds(0, peers)]
    pltpu.make_async_copy(all_asked, all_asked, asked_recv).wait()
    pltpu.make_async_copy(all_asked, all_asked, asked_send).wait()
    to_scalar = pltpu.make_async_copy(asked_v, asked_s, asked_copy)
    to_scalar.start()
    to_scalar.wait()

    relay_sums(0)
    for s in range(STREAMS):
        relay(0, s, EARLY[1:])
        if s < STREAMS - 1:
            relay(0, s, LATE)
    adj_copy.wait()
    left = (0, STREAMS - 1)

    for h in range(HOPS):
        p = (h + 1) % 2
        for s in range(STREAMS):
            finish(h, s)
            if h < HOPS - 1:
                relay(p, s, HEAD)
            if left is not None:
                relay(*left, LATE)
                left = None
            if h < HOPS - 1:
                relay(p, s, EARLY)
                left = (p, s)
                if h == HOPS - 2 and s == STREAMS - 1:
                    relay(p, s, LATE)
                    left = None


def local(adjacency_tiles, col_block, label_prior, seed_label, seed_mask):
    blocks_dev, degree, block_rows, _ = adjacency_tiles.shape
    nodes, classes = label_prior.shape
    n_rows = lax.axis_size("rows")
    n_cols = lax.axis_size("cols")
    group = n_cols * blocks_dev
    lanes = classes // STREAMS
    padded = -(-n_rows // LANES) * LANES
    pairs = max(n_cols // 2, 2)
    span = (pairs - 1) * 2 * blocks_dev
    others = max(n_cols - 1, 1)
    unit = block_rows // sum(CHUNK_PARTS)
    dma = pltpu.SemaphoreType.DMA
    vmem = pl.BlockSpec(memory_space=pltpu.VMEM)
    return pl.pallas_call(
        functools.partial(kernel, n_rows, n_cols, blocks_dev, degree, block_rows, classes),
        out_shape=jax.ShapeDtypeStruct((nodes, classes), jnp.float32),
        in_specs=[
            pl.BlockSpec(memory_space=pl.ANY),
        ] * 5,
        out_specs=vmem,
        scratch_shapes=[
            [
                [
                    [
                        pltpu.VMEM((group + n_rows, unit * part, lanes), jnp.bfloat16)
                        for part in CHUNK_PARTS
                    ]
                    for _ in range(STREAMS)
                ]
                for _ in range(2)
            ],
            pltpu.VMEM((2, STREAMS, n_rows, block_rows, lanes), jnp.bfloat16),
            pltpu.VMEM((STREAMS, 2, n_rows, block_rows, lanes), jnp.bfloat16),
            [
                [
                    [pltpu.VMEM((span, unit * part // 2, lanes), jnp.bfloat16) for part in CHUNK_PARTS]
                    for _ in range(STREAMS)
                ]
                for _ in range(2)
            ],
            [pltpu.VMEM((group + n_rows, 1, block_rows), jnp.float32) for _ in range(2)],
            pltpu.VMEM((2, n_rows, 1, block_rows), jnp.float32),
            pltpu.VMEM((n_rows, 1, block_rows), jnp.float32),
            pltpu.VMEM((blocks_dev, 1, block_rows), jnp.float32),
            pltpu.VMEM((nodes, lanes), jnp.float32),
            pltpu.VMEM((nodes, lanes), jnp.float32),
            pltpu.VMEM(adjacency_tiles.shape, jnp.bfloat16),
            pltpu.VMEM((nodes, classes), jnp.float32),
            pltpu.SMEM((blocks_dev * degree,), jnp.int32),
            pltpu.VMEM((1, padded), jnp.int32),
            pltpu.VMEM((2, n_rows, 1, padded), jnp.int32),
            pltpu.SMEM((2, n_rows, 1, padded), jnp.int32),
            pltpu.SMEM(col_block.shape, jnp.int32),
            pltpu.VMEM((nodes, classes), jnp.float32),
            pltpu.VMEM((blocks_dev, block_rows), jnp.int32),
            pltpu.VMEM((blocks_dev, block_rows), jnp.int32),
            dma((4,)),
            dma, dma, dma, dma,
            dma((2, STREAMS, CHUNKS)), dma((2, STREAMS, CHUNKS)),
            dma((2, STREAMS, pairs - 1, CHUNKS, 2)), dma((2, STREAMS, pairs - 1, CHUNKS, 2)),
            dma((2, STREAMS, pairs - 1, CHUNKS)), dma((2, STREAMS, pairs - 1, CHUNKS)),
            dma((2, STREAMS)), dma((2, STREAMS)),
            dma((2, others)), dma((2, others)),
            dma((2,)), dma((2,)),
        ],
        compiler_params=pltpu.CompilerParams(
            collective_id=0, has_side_effects=True, vmem_limit_bytes=VMEM_LIMIT - 4 * nodes * classes - SPARE
        ),
    )(
        col_block,
        label_prior,
        seed_label.reshape(blocks_dev, block_rows),
        seed_mask.reshape(blocks_dev, block_rows),
        adjacency_tiles,
    )


def solution(mesh):
    in_specs = (
        P(("rows", "cols"), None, None, None),
        P(("rows", "cols"), None),
        P(("rows", "cols"), None),
        P(("rows", "cols")),
        P(("rows", "cols")),
    )
    out_specs = P(("rows", "cols"), None)
    return jax.shard_map(local, mesh=mesh, in_specs=in_specs, out_specs=out_specs, check_vma=False)
```

```python
import functools

import jax
import jax.numpy as jnp
from jax import lax
from jax.experimental import pallas as pl
from jax.experimental.pallas import tpu as pltpu
from jax.sharding import PartitionSpec as P

HOPS = 4
STREAMS = 2
CHUNK_PARTS = (2, 2, 4)
EARLY = "A0 A1".split()
LATE = "A2".split()
BETWEEN = ("M0 M1 A0 A1".split(), "U M0 A0 M1 A1".split())
CHUNKS = len(CHUNK_PARTS)
HEAD = [f"G{q}" for q in range(CHUNKS)]
ALPHA = 0.85
SEED_BOOST = 8.0
LANES = 128
VMEM_LIMIT = 67_043_328
SPARE = 64 * 1024
MESH = pl.DeviceIdType.MESH
PEER_ORDER = (5, 4, 7, 6, 3, 2, 1)


def kernel(
    n_rows, n_cols, blocks_dev, degree, block_rows, classes,
    col_block_hbm, prior_hbm, label_hbm, mask_hbm, adj_hbm, out_ref,
    tables, remote, reply, landed, sums, sums_remote, sums_reply, sums_part, scale_ref, blend_ref, adj_q,
    adj, anchor_ref, index_ref, wanted_ref, asked_v, asked_s,
    col_block_ref, prior_ref, label_ref, mask_ref, in_sem,
    adj_sem, asked_send, asked_recv, asked_copy,
    near_send, near_recv, far_send, far_recv, fwd_send, fwd_recv, rep_send, rep_recv,
    sums_send, sums_recv, srep_send, srep_recv,
):
    row = lax.axis_index("rows")
    col = lax.axis_index("cols")
    group = n_cols * blocks_dev
    lanes = classes // STREAMS
    pairs = n_cols // 2
    pair, low = col // 2, col % 2
    mate = pair * 2 + 1 - low
    unit = block_rows // sum(CHUNK_PARTS)
    starts = [unit * sum(CHUNK_PARTS[:q]) for q in range(CHUNKS)]
    sizes = [unit * part for part in CHUNK_PARTS]
    halves = [size // 2 for size in sizes]
    peers = n_rows - 1

    def each_peer(body):
        if n_rows <= 8 and n_rows & (n_rows - 1) == 0:
            for flips in PEER_ORDER:
                if flips < n_rows:
                    other = row
                    for i in range(3):
                        if flips >> i & 1:
                            other = other + (1 << i) * (1 - 2 * ((row // (1 << i)) % 2))
                    body(other)
            return
        half = n_rows // 2
        def step(i):
            if isinstance(i, int):
                d = half + ((i + 1) // 2) * (1 - 2 * (i % 2))
            else:
                d = half + lax.div(i + 1, 2) * (1 - 2 * lax.rem(i, 2))
            body((row + d + n_rows) % n_rows)
        if n_rows <= 8:
            for i in range(peers):
                step(i)
        else:
            def loop(i, carry):
                step(i)
                return carry
            lax.fori_loop(0, peers, loop, 0)

    adj_copy = pltpu.make_async_copy(adj_hbm, adj, adj_sem)
    loads = [
        pltpu.make_async_copy(source, target, in_sem.at[i])
        for i, (source, target) in enumerate([
            (col_block_hbm, col_block_ref),
            (label_hbm, label_ref),
            (mask_hbm, mask_ref),
            (prior_hbm, prior_ref),
        ])
    ]
    for load in loads:
        load.start()
    adj_copy.start()

    barrier = pltpu.get_barrier_semaphore()
    for j in range(1, n_cols):
        pl.semaphore_signal(
            barrier, inc=1, device_id=(row, (col + j) % n_cols), device_id_type=MESH
        )
    def greet(other):
        for r in range(2):
            pl.semaphore_signal(
                barrier, inc=1, device_id=(other, pair * 2 + r), device_id_type=MESH
            )

    each_peer(greet)

    ones = jnp.ones((8, lanes), jnp.bfloat16)

    def keep(p, s, b, labels):
        sent = labels.astype(jnp.bfloat16)
        for q in range(CHUNKS):
            tables[p][s][q][col * blocks_dev + b] = sent[starts[q] : starts[q] + sizes[q], :]

    def sum_rows(p, s):
        for b in range(blocks_dev):
            mine = col * blocks_dev + b
            sent = jnp.concatenate([tables[p][s][q][mine] for q in range(CHUNKS)], axis=0)
            total = lax.dot_general(
                ones, sent, (((1,), (1,)), ((), ())), preferred_element_type=jnp.float32
            )[:1, :]
            if s > 0:
                total = total + sums_part[b]
            if s < STREAMS - 1:
                sums_part[b] = total
            else:
                sums[p][mine] = total

    loads[0].wait()
    lane = lax.broadcasted_iota(jnp.int32, wanted_ref.shape, 1)
    wanted = jnp.zeros(wanted_ref.shape, jnp.int32)
    for b in range(blocks_dev):
        for k in range(degree):
            block = col_block_ref[b, k]
            owner = lax.div(block, group)
            within = block - owner * group
            index_ref[b * degree + k] = jnp.where(owner == row, within, group + owner)
            wanted = jnp.where(lane == owner, within, wanted)
    wanted_ref[...] = wanted

    pl.semaphore_wait(barrier, n_cols - 1 + 2 * peers)

    def send_wanted(other):
        for r in range(2):
            pltpu.make_async_remote_copy(
                src_ref=wanted_ref, dst_ref=asked_v.at[low, row],
                send_sem=asked_send, recv_sem=asked_recv,
                device_id=(other, pair * 2 + r), device_id_type=MESH,
            ).start()

    each_peer(send_wanted)

    for load in loads[1:]:
        load.wait()
    code = jnp.where(mask_ref[...] > 0, label_ref[...], -1)
    for b in range(blocks_dev):
        here = slice(b * block_rows, (b + 1) * block_rows)
        across = jnp.broadcast_to(code[b : b + 1, :], (block_rows, block_rows)).T
        class_id = lax.broadcasted_iota(jnp.int32, (block_rows, classes), 1)
        across = jnp.concatenate([across] * (classes // block_rows), axis=1)
        raw = prior_ref[here, :] + jnp.where(class_id == across, SEED_BOOST, 0.0)
        anchor = raw * (classes / jnp.sum(raw, axis=1, keepdims=True))
        anchor_ref[here, :] = anchor
        for s in range(STREAMS):
            keep(0, s, b, anchor[:, s * lanes : (s + 1) * lanes])

    def rows_of(q, r):
        return pl.ds(pl.multiple_of(r * halves[q], 8), halves[q])

    def near(p, s, q):
        ref = tables[p][s][q].at[pl.ds(col * blocks_dev, blocks_dev)]
        return pltpu.make_async_remote_copy(
            src_ref=ref, dst_ref=ref,
            send_sem=near_send.at[p, s, q], recv_sem=near_recv.at[p, s, q],
            device_id=(row, mate), device_id_type=MESH,
        )

    def far(p, s, j, q, d):
        r = (low + d) % 2
        ref = tables[p][s][q].at[pl.ds(col * blocks_dev, blocks_dev), rows_of(q, r), :]
        return pltpu.make_async_remote_copy(
            src_ref=ref, dst_ref=ref,
            send_sem=far_send.at[p, s, j - 1, q, d], recv_sem=far_recv.at[p, s, j - 1, q, d],
            device_id=(row, ((pair + j) % pairs) * 2 + r), device_id_type=MESH,
        )

    def forward(p, s, j, q):
        first = ((pair + pairs - j) % pairs) * 2 * blocks_dev
        return pltpu.make_async_remote_copy(
            src_ref=tables[p][s][q].at[pl.ds(first, 2 * blocks_dev), rows_of(q, low), :],
            dst_ref=landed[p][s][q].at[pl.ds((j - 1) * 2 * blocks_dev, 2 * blocks_dev)],
            send_sem=fwd_send.at[p, s, j - 1, q], recv_sem=fwd_recv.at[p, s, j - 1, q],
            device_id=(row, mate), device_id_type=MESH,
        )

    def sums_to(p, j):
        ref = sums[p].at[pl.ds(col * blocks_dev, blocks_dev)]
        return pltpu.make_async_remote_copy(
            src_ref=ref, dst_ref=ref,
            send_sem=sums_send.at[p, j - 1], recv_sem=sums_recv.at[p, j - 1],
            device_id=(row, (col + j) % n_cols), device_id_type=MESH,
        )

    def start_sums(p):
        for j in range(1, n_cols):
            sums_to(p, j).start()

    def start_gather(p, s, q):
        for j in range(1, pairs):
            for d in range(2):
                far(p, s, j, q, d).start()
        near(p, s, q).start()

    def relay_sums(p):
        for j in range(1, n_cols):
            sums_to(p, j).wait_recv()

        def answer(other):
            sums_reply[other] = sums[p][asked_s[low, other, 0, row]]
            pltpu.make_async_remote_copy(
                src_ref=sums_reply.at[other], dst_ref=sums_remote.at[p, row],
                send_sem=srep_send.at[p], recv_sem=srep_recv.at[p],
                device_id=(other, col), device_id_type=MESH,
            ).start()

        each_peer(answer)

    def relay(p, s, steps):
        for kind, q in [(text[0], int(text[1:] or 0)) for text in steps]:
            if kind == "G":
                start_gather(p, s, q)
                continue
            if kind == "S":
                sum_rows(p, s)
                if s == STREAMS - 1:
                    start_sums(p)
                continue
            if kind == "U":
                if s == STREAMS - 1:
                    relay_sums(p)
                continue
            for j in range(1, pairs):
                for d in range(2):
                    far(p, s, j, q, d).wait_recv()
            near(p, s, q).wait_recv()
            rows_q = pl.ds(pl.multiple_of(starts[q] + low * halves[q], 8), halves[q])

            def answer(other):
                for r in range(2):
                    reply[s, r, other, rows_q, :] = tables[p][s][q][
                        asked_s[r, other, 0, row], rows_of(q, low), :
                    ]
                    pltpu.make_async_remote_copy(
                        src_ref=reply.at[s, r, other, rows_q, :],
                        dst_ref=remote.at[p, s, row, rows_q, :],
                        send_sem=rep_send.at[p, s], recv_sem=rep_recv.at[p, s, q],
                        device_id=(other, pair * 2 + r), device_id_type=MESH,
                    ).start()

            each_peer(answer)
            for j in range(1, pairs):
                forward(p, s, j, q).start()

    def product(p, s, b, q):
        rhs = [tables[p][s][q][index_ref[b * degree + k]] for k in range(degree)]
        return jnp.dot(
            adj_q[q][b], jnp.concatenate(rhs, axis=0), preferred_element_type=jnp.float32
        )

    def row_scale(p, b):
        here = slice(b * block_rows, (b + 1) * block_rows)
        total = jnp.zeros((block_rows, block_rows), jnp.float32)
        for k in range(degree):
            total = total + adj[b, k].astype(jnp.float32) * sums[p][index_ref[b * degree + k]]
        rest = anchor_ref[here, :block_rows]
        for i in range(1, classes // block_rows):
            rest = rest + anchor_ref[here, i * block_rows : (i + 1) * block_rows]
        total = ALPHA * total + (1.0 - ALPHA) * rest
        return classes / jnp.sum(total, axis=1, keepdims=True)

    def blend(p, s, b, q, mine):
        here = slice(b * block_rows, (b + 1) * block_rows)
        spread = product(p, s, b, q)
        if q > 0:
            spread = spread + blend_ref[s, here, :]
        if q < CHUNKS - 1:
            return spread
        return ALPHA * spread + (1.0 - ALPHA) * anchor_ref[here, mine]

    blended = {}

    def gathered(p, s, q):
        rows_q = pl.ds(starts[q], sizes[q])
        got = remote.at[p, s, pl.ds(0, peers), rows_q, :]
        pltpu.make_async_copy(got, got, rep_recv.at[p, s, q]).wait()
        for j in range(1, pairs):
            forward(p, s, j, q).wait_recv()
            first = ((pair + pairs - j) % pairs) * 2 * blocks_dev
            tables[p][s][q][pl.ds(first, 2 * blocks_dev), rows_of(q, 1 - low), :] = landed[p][s][q][
                pl.ds((j - 1) * 2 * blocks_dev, 2 * blocks_dev)
            ]

        def fold(other):
            tables[p][s][q][group + other] = remote[p, s, other, rows_q, :]

        each_peer(fold)

    def partial(h, s, q):
        p = h % 2
        gathered(p, s, q)
        for b in range(blocks_dev):
            here = slice(b * block_rows, (b + 1) * block_rows)
            blend_ref[s, here, :] = blend(p, s, b, q, slice(s * lanes, (s + 1) * lanes))
        blended[h, s] = q + 1

    def finish(h, s):
        p, last = h % 2, h == HOPS - 1
        mine = slice(s * lanes, (s + 1) * lanes)
        for q in range(blended.get((h, s), 0), CHUNKS - (s > 0)):
            partial(h, s, q)
        if s > 0:
            gathered(p, s, CHUNKS - 1)

        if s == 0:
            got = sums_remote.at[p, pl.ds(0, peers)]
            pltpu.make_async_copy(got, got, srep_recv.at[p]).wait()

            def fold_sums(other):
                sums[p][group + other] = sums_remote[p, other]

            each_peer(fold_sums)

        for b in range(blocks_dev):
            here = slice(b * block_rows, (b + 1) * block_rows)
            if s == 0:
                scale = jnp.broadcast_to(row_scale(p, b), (block_rows, lanes))
                scale_ref[here, :] = scale
                labels = blend_ref[s, here, :] * scale
            else:
                labels = blend(p, s, b, CHUNKS - 1, mine) * scale_ref[here, :]
            if last:
                out_ref[here, mine] = labels
            else:
                keep(1 - p, s, b, labels)

        for q in range(CHUNKS):
            for j in range(1, pairs):
                for d in range(2):
                    far(p, s, j, q, d).wait_send()
                forward(p, s, j, q).wait_send()
            near(p, s, q).wait_send()
        for r in range(2):
            sent = reply.at[s, r, pl.ds(0, peers), pl.ds(0, block_rows // 2), :]
            pltpu.make_async_copy(sent, sent, rep_send.at[p, s]).wait()
        if s == STREAMS - 1:
            for j in range(1, n_cols):
                sums_to(p, j).wait_send()
            sent = sums_reply.at[pl.ds(0, peers)]
            pltpu.make_async_copy(sent, sent, srep_send.at[p]).wait()


    for s in range(STREAMS):
        relay(0, s, ["S"])
    for s in range(STREAMS):
        relay(0, s, HEAD)

    all_asked = asked_v.at[:, pl.ds(0, peers)]
    pltpu.make_async_copy(all_asked, all_asked, asked_recv).wait()
    pltpu.make_async_copy(all_asked, all_asked, asked_send).wait()
    to_scalar = pltpu.make_async_copy(asked_v, asked_s, asked_copy)
    to_scalar.start()
    to_scalar.wait()

    relay_sums(0)
    for s in range(STREAMS):
        relay(0, s, EARLY)
        if s < STREAMS - 1:
            relay(0, s, LATE)
    adj_copy.wait()
    for b in range(blocks_dev):
        for q in range(CHUNKS):
            columns = slice(starts[q], starts[q] + sizes[q])
            adj_q[q][b] = jnp.concatenate([adj[b, k][:, columns] for k in range(degree)], axis=1)
    left = (0, STREAMS - 1)

    for h in range(HOPS):
        p = (h + 1) % 2
        for s in range(STREAMS):
            finish(h, s)
            if h < HOPS - 1:
                relay(p, s, ["S"] + HEAD if s == STREAMS - 1 else HEAD + ["S"])
            if left is not None:
                relay(*left, LATE)
                left = None
            if h < HOPS - 1:
                pending = (h, s + 1) if s < STREAMS - 1 else (h + 1, 0)
                for text in BETWEEN[s > 0]:
                    if text[0] == "M":
                        partial(*pending, int(text[1:]))
                    else:
                        relay(p, s, [text])
                left = (p, s)
                if h == HOPS - 2 and s == STREAMS - 1:
                    relay(p, s, LATE)
                    left = None


def local(adjacency_tiles, col_block, label_prior, seed_label, seed_mask):
    blocks_dev, degree, block_rows, _ = adjacency_tiles.shape
    nodes, classes = label_prior.shape
    n_rows = lax.axis_size("rows")
    n_cols = lax.axis_size("cols")
    group = n_cols * blocks_dev
    lanes = classes // STREAMS
    padded = -(-n_rows // LANES) * LANES
    pairs = max(n_cols // 2, 2)
    span = (pairs - 1) * 2 * blocks_dev
    others = max(n_cols - 1, 1)
    unit = block_rows // sum(CHUNK_PARTS)
    dma = pltpu.SemaphoreType.DMA
    vmem = pl.BlockSpec(memory_space=pltpu.VMEM)
    return pl.pallas_call(
        functools.partial(kernel, n_rows, n_cols, blocks_dev, degree, block_rows, classes),
        out_shape=jax.ShapeDtypeStruct((nodes, classes), jnp.float32),
        in_specs=[
            pl.BlockSpec(memory_space=pl.ANY),
        ] * 5,
        out_specs=vmem,
        scratch_shapes=[
            [
                [
                    [
                        pltpu.VMEM((group + n_rows, unit * part, lanes), jnp.bfloat16)
                        for part in CHUNK_PARTS
                    ]
                    for _ in range(STREAMS)
                ]
                for _ in range(2)
            ],
            pltpu.VMEM((2, STREAMS, n_rows, block_rows, lanes), jnp.bfloat16),
            pltpu.VMEM((STREAMS, 2, n_rows, block_rows, lanes), jnp.bfloat16),
            [
                [
                    [pltpu.VMEM((span, unit * part // 2, lanes), jnp.bfloat16) for part in CHUNK_PARTS]
                    for _ in range(STREAMS)
                ]
                for _ in range(2)
            ],
            [pltpu.VMEM((group + n_rows, 1, block_rows), jnp.float32) for _ in range(2)],
            pltpu.VMEM((2, n_rows, 1, block_rows), jnp.float32),
            pltpu.VMEM((n_rows, 1, block_rows), jnp.float32),
            pltpu.VMEM((blocks_dev, 1, block_rows), jnp.float32),
            pltpu.VMEM((nodes, lanes), jnp.float32),
            pltpu.VMEM((STREAMS, nodes, lanes), jnp.float32),
            [
                pltpu.VMEM((blocks_dev, block_rows, degree * unit * part), jnp.bfloat16)
                for part in CHUNK_PARTS
            ],
            pltpu.VMEM(adjacency_tiles.shape, jnp.bfloat16),
            pltpu.VMEM((nodes, classes), jnp.float32),
            pltpu.SMEM((blocks_dev * degree,), jnp.int32),
            pltpu.VMEM((1, padded), jnp.int32),
            pltpu.VMEM((2, n_rows, 1, padded), jnp.int32),
            pltpu.SMEM((2, n_rows, 1, padded), jnp.int32),
            pltpu.SMEM(col_block.shape, jnp.int32),
            pltpu.VMEM((nodes, classes), jnp.float32),
            pltpu.VMEM((blocks_dev, block_rows), jnp.int32),
            pltpu.VMEM((blocks_dev, block_rows), jnp.int32),
            dma((4,)),
            dma, dma, dma, dma,
            dma((2, STREAMS, CHUNKS)), dma((2, STREAMS, CHUNKS)),
            dma((2, STREAMS, pairs - 1, CHUNKS, 2)), dma((2, STREAMS, pairs - 1, CHUNKS, 2)),
            dma((2, STREAMS, pairs - 1, CHUNKS)), dma((2, STREAMS, pairs - 1, CHUNKS)),
            dma((2, STREAMS)), dma((2, STREAMS, CHUNKS)),
            dma((2, others)), dma((2, others)),
            dma((2,)), dma((2,)),
        ],
        compiler_params=pltpu.CompilerParams(
            collective_id=0, has_side_effects=True, vmem_limit_bytes=VMEM_LIMIT - 4 * nodes * classes - SPARE
        ),
    )(
        col_block,
        label_prior,
        seed_label.reshape(blocks_dev, block_rows),
        seed_mask.reshape(blocks_dev, block_rows),
        adjacency_tiles,
    )


def solution(mesh):
    in_specs = (
        P(("rows", "cols"), None, None, None),
        P(("rows", "cols"), None),
        P(("rows", "cols"), None),
        P(("rows", "cols")),
        P(("rows", "cols")),
    )
    out_specs = P(("rows", "cols"), None)
    return jax.shard_map(local, mesh=mesh, in_specs=in_specs, out_specs=out_specs, check_vma=False)
```

```python
import functools

import jax
import jax.numpy as jnp
from jax import lax
from jax.experimental import pallas as pl
from jax.experimental.pallas import tpu as pltpu
from jax.sharding import PartitionSpec as P

HOPS = 4
STREAMS = 2
CHUNK_PARTS = (2, 2, 4)
EARLY = ("A0", "A1")
LATE = ("A2",)
BETWEEN = (("M0", "M1", "A0", "A1"), ("U", "M0", "A0", "M1", "A1"))
CHUNKS = len(CHUNK_PARTS)
HEAD = [f"G{q}" for q in range(CHUNKS)]
ALPHA = 0.85
SEED_BOOST = 8.0
LANES = 128
VMEM_LIMIT = 67_043_328
SPARE = 64 * 1024
MESH = pl.DeviceIdType.MESH
PEER_ORDER = (5, 4, 7, 6, 3, 2, 1)


def kernel(
    n_rows, n_cols, blocks_dev, degree, block_rows, classes,
    col_block_hbm, prior_hbm, label_hbm, mask_hbm, adj_hbm, out_ref,
    tables, remote, reply, landed, sums, sums_remote, sums_reply, sums_part, scale_ref, blend_ref, adj_q,
    adj, anchor_ref, index_ref, wanted_ref, asked_v, asked_s,
    col_block_ref, prior_ref, label_ref, mask_ref, in_sem,
    adj_sem, asked_send, asked_recv, asked_copy,
    near_send, near_recv, far_send, far_recv, fwd_send, fwd_recv, rep_send, rep_recv,
    sums_send, sums_recv, srep_send, srep_recv,
):
    row = lax.axis_index("rows")
    col = lax.axis_index("cols")
    group = n_cols * blocks_dev
    lanes = classes // STREAMS
    pairs = n_cols // 2
    pair, low = col // 2, col % 2
    mate = pair * 2 + 1 - low
    unit = block_rows // sum(CHUNK_PARTS)
    starts = [unit * sum(CHUNK_PARTS[:q]) for q in range(CHUNKS)]
    sizes = [unit * part for part in CHUNK_PARTS]
    halves = [size // 2 for size in sizes]
    peers = n_rows - 1

    def each_peer(body):
        if n_rows <= 8 and n_rows & (n_rows - 1) == 0:
            for flips in PEER_ORDER:
                if flips < n_rows:
                    other = row
                    for i in range(3):
                        if flips >> i & 1:
                            other = other + (1 << i) * (1 - 2 * ((row // (1 << i)) % 2))
                    body(other)
            return
        half = n_rows // 2
        def step(i):
            if isinstance(i, int):
                d = half + ((i + 1) // 2) * (1 - 2 * (i % 2))
            else:
                d = half + lax.div(i + 1, 2) * (1 - 2 * lax.rem(i, 2))
            body((row + d + n_rows) % n_rows)
        if n_rows <= 8:
            for i in range(peers):
                step(i)
        else:
            def loop(i, carry):
                step(i)
                return carry
            lax.fori_loop(0, peers, loop, 0)

    adj_copy = pltpu.make_async_copy(adj_hbm, adj, adj_sem)
    loads = [
        pltpu.make_async_copy(source, target, in_sem.at[i])
        for i, (source, target) in enumerate([
            (col_block_hbm, col_block_ref),
            (label_hbm, label_ref),
            (mask_hbm, mask_ref),
            (prior_hbm, prior_ref),
        ])
    ]
    for load in loads:
        load.start()
    adj_copy.start()

    barrier = pltpu.get_barrier_semaphore()
    for j in range(1, n_cols):
        pl.semaphore_signal(
            barrier, inc=1, device_id=(row, (col + j) % n_cols), device_id_type=MESH
        )
    def greet(other):
        for r in range(2):
            pl.semaphore_signal(
                barrier, inc=1, device_id=(other, pair * 2 + r), device_id_type=MESH
            )

    each_peer(greet)

    ones = jnp.ones((8, lanes), jnp.bfloat16)

    def keep(p, s, b, labels):
        sent = labels.astype(jnp.bfloat16)
        for q in range(CHUNKS):
            tables[p][s][q][col * blocks_dev + b] = sent[starts[q] : starts[q] + sizes[q], :]

    def sum_rows(p, s):
        for b in range(blocks_dev):
            mine = col * blocks_dev + b
            sent = jnp.concatenate([tables[p][s][q][mine] for q in range(CHUNKS)], axis=0)
            total = lax.dot_general(
                ones, sent, (((1,), (1,)), ((), ())), preferred_element_type=jnp.float32
            )[:1, :]
            if s > 0:
                total = total + sums_part[b]
            if s < STREAMS - 1:
                sums_part[b] = total
            else:
                sums[p][mine] = total

    loads[0].wait()
    lane = lax.broadcasted_iota(jnp.int32, wanted_ref.shape, 1)
    wanted = jnp.zeros(wanted_ref.shape, jnp.int32)
    for b in range(blocks_dev):
        for k in range(degree):
            block = col_block_ref[b, k]
            owner = lax.div(block, group)
            within = block - owner * group
            index_ref[b * degree + k] = jnp.where(owner == row, within, group + owner)
            wanted = jnp.where(lane == owner, within, wanted)
    wanted_ref[...] = wanted

    pl.semaphore_wait(barrier, n_cols - 1 + 2 * peers)

    def send_wanted(other):
        for r in range(2):
            pltpu.make_async_remote_copy(
                src_ref=wanted_ref, dst_ref=asked_v.at[low, row],
                send_sem=asked_send, recv_sem=asked_recv,
                device_id=(other, pair * 2 + r), device_id_type=MESH,
            ).start()

    each_peer(send_wanted)

    for load in loads[1:]:
        load.wait()
    code = jnp.where(mask_ref[...] > 0, label_ref[...], -1)
    for b in range(blocks_dev):
        here = slice(b * block_rows, (b + 1) * block_rows)
        across = jnp.broadcast_to(code[b : b + 1, :], (block_rows, block_rows)).T
        class_id = lax.broadcasted_iota(jnp.int32, (block_rows, classes), 1)
        across = jnp.concatenate([across] * (classes // block_rows), axis=1)
        raw = prior_ref[here, :] + jnp.where(class_id == across, SEED_BOOST, 0.0)
        anchor = raw * (classes / jnp.sum(raw, axis=1, keepdims=True))
        anchor_ref[here, :] = anchor
        for s in range(STREAMS):
            keep(0, s, b, anchor[:, s * lanes : (s + 1) * lanes])

    def rows_of(q, r):
        return pl.ds(pl.multiple_of(r * halves[q], 8), halves[q])

    def near(p, s, q):
        ref = tables[p][s][q].at[pl.ds(col * blocks_dev, blocks_dev)]
        return pltpu.make_async_remote_copy(
            src_ref=ref, dst_ref=ref,
            send_sem=near_send.at[p, s, q], recv_sem=near_recv.at[p, s, q],
            device_id=(row, mate), device_id_type=MESH,
        )

    def far(p, s, j, q, d):
        r = (low + d) % 2
        ref = tables[p][s][q].at[pl.ds(col * blocks_dev, blocks_dev), rows_of(q, r), :]
        return pltpu.make_async_remote_copy(
            src_ref=ref, dst_ref=ref,
            send_sem=far_send.at[p, s, j - 1, q, d], recv_sem=far_recv.at[p, s, j - 1, q, d],
            device_id=(row, ((pair + j) % pairs) * 2 + r), device_id_type=MESH,
        )

    def forward(p, s, j, q):
        first = ((pair + pairs - j) % pairs) * 2 * blocks_dev
        return pltpu.make_async_remote_copy(
            src_ref=tables[p][s][q].at[pl.ds(first, 2 * blocks_dev), rows_of(q, low), :],
            dst_ref=landed[p][s][q].at[pl.ds((j - 1) * 2 * blocks_dev, 2 * blocks_dev)],
            send_sem=fwd_send.at[p, s, j - 1, q], recv_sem=fwd_recv.at[p, s, j - 1, q],
            device_id=(row, mate), device_id_type=MESH,
        )

    def sums_near(p):
        ref = sums[p].at[pl.ds(col * blocks_dev, blocks_dev)]
        return pltpu.make_async_remote_copy(
            src_ref=ref, dst_ref=ref, send_sem=sums_send.at[p, 0], recv_sem=sums_recv.at[p, 0],
            device_id=(row, mate), device_id_type=MESH,
        )

    def sums_far(p, j, d):
        ref = sums[p].at[pl.ds(col * blocks_dev, blocks_dev)]
        return pltpu.make_async_remote_copy(
            src_ref=ref, dst_ref=ref,
            send_sem=sums_send.at[p, j], recv_sem=sums_recv.at[p, 2 * j - 1 + d],
            device_id=(row, ((pair + j) % pairs) * 2 + 1), device_id_type=MESH,
        )

    def sums_forward(p, j):
        first = ((pair + pairs - j) % pairs) * 2 * blocks_dev
        ref = sums[p].at[pl.ds(first, 2 * blocks_dev)]
        return pltpu.make_async_remote_copy(
            src_ref=ref, dst_ref=ref,
            send_sem=sums_send.at[p, pairs - 1 + j], recv_sem=sums_recv.at[p, 2 * (pairs - 1) + j],
            device_id=(row, mate), device_id_type=MESH,
        )

    def start_sums(p):
        for j in range(1, pairs):
            sums_far(p, j, low).start()
        sums_near(p).start()

    def start_gather(p, s, q):
        for j in range(1, pairs):
            for d in range(2):
                far(p, s, j, q, d).start()
        near(p, s, q).start()

    def relay_sums(p):
        sums_near(p).wait_recv()

        @pl.when(low == 1)
        def _():
            for j in range(1, pairs):
                for d in range(2):
                    sums_far(p, j, d).wait_recv()

            def answer(other):
                for r in range(2):
                    sums_reply[r, other] = sums[p][asked_s[r, other, 0, row]]
                    pltpu.make_async_remote_copy(
                        src_ref=sums_reply.at[r, other], dst_ref=sums_remote.at[p, row],
                        send_sem=srep_send.at[p], recv_sem=srep_recv.at[p],
                        device_id=(other, pair * 2 + r), device_id_type=MESH,
                    ).start()

            each_peer(answer)
            for j in range(1, pairs):
                sums_forward(p, j).start()

    def relay(p, s, steps):
        for kind, q in [(text[0], int(text[1:] or 0)) for text in steps]:
            if kind == "G":
                start_gather(p, s, q)
                continue
            if kind == "S":
                sum_rows(p, s)
                if s == STREAMS - 1:
                    start_sums(p)
                continue
            if kind == "U":
                if s == STREAMS - 1:
                    relay_sums(p)
                continue
            for j in range(1, pairs):
                for d in range(2):
                    far(p, s, j, q, d).wait_recv()
            near(p, s, q).wait_recv()
            rows_q = pl.ds(pl.multiple_of(starts[q] + low * halves[q], 8), halves[q])

            def answer(other):
                for r in range(2):
                    reply[s, r, other, rows_q, :] = tables[p][s][q][
                        asked_s[r, other, 0, row], rows_of(q, low), :
                    ]
                    pltpu.make_async_remote_copy(
                        src_ref=reply.at[s, r, other, rows_q, :],
                        dst_ref=remote.at[p, s, row, rows_q, :],
                        send_sem=rep_send.at[p, s], recv_sem=rep_recv.at[p, s, q],
                        device_id=(other, pair * 2 + r), device_id_type=MESH,
                    ).start()

            each_peer(answer)
            for j in range(1, pairs):
                forward(p, s, j, q).start()

    def product(p, s, b, q):
        rhs = [tables[p][s][q][index_ref[b * degree + k]] for k in range(degree)]
        return jnp.dot(
            adj_q[q][b], jnp.concatenate(rhs, axis=0), preferred_element_type=jnp.float32
        )

    def row_scale(p, b):
        here = slice(b * block_rows, (b + 1) * block_rows)
        total = jnp.zeros((block_rows, block_rows), jnp.float32)
        for k in range(degree):
            total = total + adj[b, k].astype(jnp.float32) * sums[p][index_ref[b * degree + k]]
        rest = anchor_ref[here, :block_rows]
        for i in range(1, classes // block_rows):
            rest = rest + anchor_ref[here, i * block_rows : (i + 1) * block_rows]
        total = ALPHA * total + (1.0 - ALPHA) * rest
        return classes / jnp.sum(total, axis=1, keepdims=True)

    def blend(p, s, b, q, mine):
        here = slice(b * block_rows, (b + 1) * block_rows)
        spread = product(p, s, b, q)
        if q > 0:
            spread = spread + blend_ref[s, here, :]
        if q < CHUNKS - 1:
            return spread
        return ALPHA * spread + (1.0 - ALPHA) * anchor_ref[here, mine]

    blended = {}

    def gathered(p, s, q):
        rows_q = pl.ds(starts[q], sizes[q])
        got = remote.at[p, s, pl.ds(0, peers), rows_q, :]
        pltpu.make_async_copy(got, got, rep_recv.at[p, s, q]).wait()
        for j in range(1, pairs):
            forward(p, s, j, q).wait_recv()
            first = ((pair + pairs - j) % pairs) * 2 * blocks_dev
            tables[p][s][q][pl.ds(first, 2 * blocks_dev), rows_of(q, 1 - low), :] = landed[p][s][q][
                pl.ds((j - 1) * 2 * blocks_dev, 2 * blocks_dev)
            ]

        def fold(other):
            tables[p][s][q][group + other] = remote[p, s, other, rows_q, :]

        each_peer(fold)

    def partial(h, s, q):
        p = h % 2
        gathered(p, s, q)
        for b in range(blocks_dev):
            here = slice(b * block_rows, (b + 1) * block_rows)
            blend_ref[s, here, :] = blend(p, s, b, q, slice(s * lanes, (s + 1) * lanes))
        blended[h, s] = q + 1

    def finish(h, s):
        p, last = h % 2, h == HOPS - 1
        mine = slice(s * lanes, (s + 1) * lanes)
        for q in range(blended.get((h, s), 0), CHUNKS - (s > 0)):
            partial(h, s, q)
        if s > 0:
            gathered(p, s, CHUNKS - 1)

        if s == 0:
            got = sums_remote.at[p, pl.ds(0, peers)]
            pltpu.make_async_copy(got, got, srep_recv.at[p]).wait()

            @pl.when(low == 0)
            def _():
                for j in range(1, pairs):
                    sums_forward(p, j).wait_recv()

            def fold_sums(other):
                sums[p][group + other] = sums_remote[p, other]

            each_peer(fold_sums)

        for b in range(blocks_dev):
            here = slice(b * block_rows, (b + 1) * block_rows)
            if s == 0:
                scale = jnp.broadcast_to(row_scale(p, b), (block_rows, lanes))
                scale_ref[here, :] = scale
                labels = blend_ref[s, here, :] * scale
            else:
                labels = blend(p, s, b, CHUNKS - 1, mine) * scale_ref[here, :]
            if last:
                out_ref[here, mine] = labels
            else:
                keep(1 - p, s, b, labels)

        for q in range(CHUNKS):
            for j in range(1, pairs):
                for d in range(2):
                    far(p, s, j, q, d).wait_send()
                forward(p, s, j, q).wait_send()
            near(p, s, q).wait_send()
        for r in range(2):
            sent = reply.at[s, r, pl.ds(0, peers), pl.ds(0, block_rows // 2), :]
            pltpu.make_async_copy(sent, sent, rep_send.at[p, s]).wait()
        if s == STREAMS - 1:
            for j in range(1, pairs):
                sums_far(p, j, low).wait_send()
            sums_near(p).wait_send()

            @pl.when(low == 1)
            def _():
                sent = sums_reply.at[:, pl.ds(0, peers)]
                pltpu.make_async_copy(sent, sent, srep_send.at[p]).wait()
                for j in range(1, pairs):
                    sums_forward(p, j).wait_send()


    for s in range(STREAMS):
        relay(0, s, ["S"])
    for s in range(STREAMS):
        relay(0, s, HEAD)

    all_asked = asked_v.at[:, pl.ds(0, peers)]
    pltpu.make_async_copy(all_asked, all_asked, asked_recv).wait()
    pltpu.make_async_copy(all_asked, all_asked, asked_send).wait()
    to_scalar = pltpu.make_async_copy(asked_v, asked_s, asked_copy)
    to_scalar.start()
    to_scalar.wait()

    relay_sums(0)
    for s in range(STREAMS):
        relay(0, s, EARLY)
        if s < STREAMS - 1:
            relay(0, s, LATE)
    adj_copy.wait()
    for b in range(blocks_dev):
        for q in range(CHUNKS):
            columns = slice(starts[q], starts[q] + sizes[q])
            adj_q[q][b] = jnp.concatenate([adj[b, k][:, columns] for k in range(degree)], axis=1)
    left = (0, STREAMS - 1)

    for h in range(HOPS):
        p = (h + 1) % 2
        for s in range(STREAMS):
            finish(h, s)
            if h < HOPS - 1:
                relay(p, s, ["S"] + HEAD if s == STREAMS - 1 else HEAD + ["S"])
            if left is not None:
                relay(*left, LATE)
                left = None
            if h < HOPS - 1:
                pending = (h, s + 1) if s < STREAMS - 1 else (h + 1, 0)
                for text in BETWEEN[s > 0]:
                    if text[0] == "M":
                        partial(*pending, int(text[1:]))
                    else:
                        relay(p, s, [text])
                left = (p, s)
                if h == HOPS - 2 and s == STREAMS - 1:
                    relay(p, s, LATE)
                    left = None


def local(adjacency_tiles, col_block, label_prior, seed_label, seed_mask):
    blocks_dev, degree, block_rows, _ = adjacency_tiles.shape
    nodes, classes = label_prior.shape
    n_rows = lax.axis_size("rows")
    n_cols = lax.axis_size("cols")
    group = n_cols * blocks_dev
    lanes = classes // STREAMS
    padded = -(-n_rows // LANES) * LANES
    pairs = max(n_cols // 2, 2)
    span = (pairs - 1) * 2 * blocks_dev
    unit = block_rows // sum(CHUNK_PARTS)
    dma = pltpu.SemaphoreType.DMA
    vmem = pl.BlockSpec(memory_space=pltpu.VMEM)
    return pl.pallas_call(
        functools.partial(kernel, n_rows, n_cols, blocks_dev, degree, block_rows, classes),
        out_shape=jax.ShapeDtypeStruct((nodes, classes), jnp.float32),
        in_specs=[
            pl.BlockSpec(memory_space=pl.ANY),
        ] * 5,
        out_specs=vmem,
        scratch_shapes=[
            [
                [
                    [
                        pltpu.VMEM((group + n_rows, unit * part, lanes), jnp.bfloat16)
                        for part in CHUNK_PARTS
                    ]
                    for _ in range(STREAMS)
                ]
                for _ in range(2)
            ],
            pltpu.VMEM((2, STREAMS, n_rows, block_rows, lanes), jnp.bfloat16),
            pltpu.VMEM((STREAMS, 2, n_rows, block_rows, lanes), jnp.bfloat16),
            [
                [
                    [pltpu.VMEM((span, unit * part // 2, lanes), jnp.bfloat16) for part in CHUNK_PARTS]
                    for _ in range(STREAMS)
                ]
                for _ in range(2)
            ],
            [pltpu.VMEM((group + n_rows, 1, block_rows), jnp.float32) for _ in range(2)],
            pltpu.VMEM((2, n_rows, 1, block_rows), jnp.float32),
            pltpu.VMEM((2, n_rows, 1, block_rows), jnp.float32),
            pltpu.VMEM((blocks_dev, 1, block_rows), jnp.float32),
            pltpu.VMEM((nodes, lanes), jnp.float32),
            pltpu.VMEM((STREAMS, nodes, lanes), jnp.float32),
            [
                pltpu.VMEM((blocks_dev, block_rows, degree * unit * part), jnp.bfloat16)
                for part in CHUNK_PARTS
            ],
            pltpu.VMEM(adjacency_tiles.shape, jnp.bfloat16),
            pltpu.VMEM((nodes, classes), jnp.float32),
            pltpu.SMEM((blocks_dev * degree,), jnp.int32),
            pltpu.VMEM((1, padded), jnp.int32),
            pltpu.VMEM((2, n_rows, 1, padded), jnp.int32),
            pltpu.SMEM((2, n_rows, 1, padded), jnp.int32),
            pltpu.SMEM(col_block.shape, jnp.int32),
            pltpu.VMEM((nodes, classes), jnp.float32),
            pltpu.VMEM((blocks_dev, block_rows), jnp.int32),
            pltpu.VMEM((blocks_dev, block_rows), jnp.int32),
            dma((4,)),
            dma, dma, dma, dma,
            dma((2, STREAMS, CHUNKS)), dma((2, STREAMS, CHUNKS)),
            dma((2, STREAMS, pairs - 1, CHUNKS, 2)), dma((2, STREAMS, pairs - 1, CHUNKS, 2)),
            dma((2, STREAMS, pairs - 1, CHUNKS)), dma((2, STREAMS, pairs - 1, CHUNKS)),
            dma((2, STREAMS)), dma((2, STREAMS, CHUNKS)),
            dma((2, 2 * pairs - 1)), dma((2, 3 * pairs - 2)),
            dma((2,)), dma((2,)),
        ],
        compiler_params=pltpu.CompilerParams(
            collective_id=0, has_side_effects=True, vmem_limit_bytes=VMEM_LIMIT - 4 * nodes * classes - SPARE
        ),
    )(
        col_block,
        label_prior,
        seed_label.reshape(blocks_dev, block_rows),
        seed_mask.reshape(blocks_dev, block_rows),
        adjacency_tiles,
    )


def solution(mesh):
    in_specs = (
        P(("rows", "cols"), None, None, None),
        P(("rows", "cols"), None),
        P(("rows", "cols"), None),
        P(("rows", "cols")),
        P(("rows", "cols")),
    )
    out_specs = P(("rows", "cols"), None)
    return jax.shard_map(local, mesh=mesh, in_specs=in_specs, out_specs=out_specs, check_vma=False)
```

```python
import functools

import jax
import jax.numpy as jnp
from jax import lax
from jax.experimental import pallas as pl
from jax.experimental.pallas import tpu as pltpu
from jax.sharding import PartitionSpec as P

HOPS = 4
STREAMS = 2
CHUNK_PARTS = (2, 2, 4)
EARLY = ("A0", "A1")
LATE = ("A2",)
BETWEEN = (("M0", "M1", "A0", "A1"), ("U", "A0", "M0", "A1", "M1"))
CHUNKS = len(CHUNK_PARTS)
HEAD = [f"G{q}" for q in range(CHUNKS)]
ALPHA = 0.85
SEED_BOOST = 8.0
LANES = 128
VMEM_LIMIT = 67_043_328
SPARE = 64 * 1024
MESH = pl.DeviceIdType.MESH
PEER_ORDER = (5, 4, 7, 6, 3, 2, 1)


def kernel(
    n_rows, n_cols, blocks_dev, degree, block_rows, classes,
    col_block_hbm, prior_hbm, label_hbm, mask_hbm, adj_hbm, out_ref,
    tables, remote, reply, landed, sums, sums_remote, sums_reply, sums_part, scale_ref, blend_ref, adj_q,
    adj, anchor_ref, index_ref, wanted_ref, asked_v, asked_s,
    col_block_ref, prior_ref, label_ref, mask_ref, in_sem,
    adj_sem, asked_send, asked_recv, asked_copy,
    near_send, near_recv, far_send, far_recv, fwd_send, fwd_recv, rep_send, rep_recv,
    sums_send, sums_recv, srep_send, srep_recv,
):
    row = lax.axis_index("rows")
    col = lax.axis_index("cols")
    group = n_cols * blocks_dev
    lanes = classes // STREAMS
    pairs = n_cols // 2
    pair, low = col // 2, col % 2
    mate = pair * 2 + 1 - low
    unit = block_rows // sum(CHUNK_PARTS)
    starts = [unit * sum(CHUNK_PARTS[:q]) for q in range(CHUNKS)]
    sizes = [unit * part for part in CHUNK_PARTS]
    halves = [size // 2 for size in sizes]
    peers = n_rows - 1

    def each_peer(body):
        if n_rows <= 8 and n_rows & (n_rows - 1) == 0:
            for flips in PEER_ORDER:
                if flips < n_rows:
                    other = row
                    for i in range(3):
                        if flips >> i & 1:
                            other = other + (1 << i) * (1 - 2 * ((row // (1 << i)) % 2))
                    body(other)
            return
        half = n_rows // 2
        def step(i):
            if isinstance(i, int):
                d = half + ((i + 1) // 2) * (1 - 2 * (i % 2))
            else:
                d = half + lax.div(i + 1, 2) * (1 - 2 * lax.rem(i, 2))
            body((row + d + n_rows) % n_rows)
        if n_rows <= 8:
            for i in range(peers):
                step(i)
        else:
            def loop(i, carry):
                step(i)
                return carry
            lax.fori_loop(0, peers, loop, 0)

    adj_copy = pltpu.make_async_copy(adj_hbm, adj, adj_sem)
    loads = [
        pltpu.make_async_copy(source, target, in_sem.at[i])
        for i, (source, target) in enumerate([
            (col_block_hbm, col_block_ref),
            (label_hbm, label_ref),
            (mask_hbm, mask_ref),
            (prior_hbm, prior_ref),
        ])
    ]
    for load in loads:
        load.start()
    adj_copy.start()

    barrier = pltpu.get_barrier_semaphore()
    for j in range(1, n_cols):
        pl.semaphore_signal(
            barrier, inc=1, device_id=(row, (col + j) % n_cols), device_id_type=MESH
        )
    def greet(other):
        for r in range(2):
            pl.semaphore_signal(
                barrier, inc=1, device_id=(other, pair * 2 + r), device_id_type=MESH
            )

    each_peer(greet)

    ones = jnp.ones((8, lanes), jnp.bfloat16)

    def keep(p, s, b, labels):
        sent = labels.astype(jnp.bfloat16)
        for q in range(CHUNKS):
            tables[p][s][q][col * blocks_dev + b] = sent[starts[q] : starts[q] + sizes[q], :]

    def sum_rows(p, s):
        for b in range(blocks_dev):
            mine = col * blocks_dev + b
            sent = jnp.concatenate([tables[p][s][q][mine] for q in range(CHUNKS)], axis=0)
            total = lax.dot_general(
                ones, sent, (((1,), (1,)), ((), ())), preferred_element_type=jnp.float32
            )[:1, :]
            if s > 0:
                total = total + sums_part[b]
            if s < STREAMS - 1:
                sums_part[b] = total
            else:
                sums[p][mine] = total

    loads[0].wait()
    lane = lax.broadcasted_iota(jnp.int32, wanted_ref.shape, 1)
    wanted = jnp.zeros(wanted_ref.shape, jnp.int32)
    for b in range(blocks_dev):
        for k in range(degree):
            block = col_block_ref[b, k]
            owner = lax.div(block, group)
            within = block - owner * group
            index_ref[b * degree + k] = jnp.where(owner == row, within, group + owner)
            wanted = jnp.where(lane == owner, within, wanted)
    wanted_ref[...] = wanted

    pl.semaphore_wait(barrier, n_cols - 1 + 2 * peers)

    def send_wanted(other):
        for r in range(2):
            pltpu.make_async_remote_copy(
                src_ref=wanted_ref, dst_ref=asked_v.at[low, row],
                send_sem=asked_send, recv_sem=asked_recv,
                device_id=(other, pair * 2 + r), device_id_type=MESH,
            ).start()

    each_peer(send_wanted)

    for load in loads[1:]:
        load.wait()
    code = jnp.where(mask_ref[...] > 0, label_ref[...], -1)
    for b in range(blocks_dev):
        here = slice(b * block_rows, (b + 1) * block_rows)
        across = jnp.broadcast_to(code[b : b + 1, :], (block_rows, block_rows)).T
        class_id = lax.broadcasted_iota(jnp.int32, (block_rows, classes), 1)
        across = jnp.concatenate([across] * (classes // block_rows), axis=1)
        raw = prior_ref[here, :] + jnp.where(class_id == across, SEED_BOOST, 0.0)
        anchor = raw * (classes / jnp.sum(raw, axis=1, keepdims=True))
        anchor_ref[here, :] = anchor
        for s in range(STREAMS):
            keep(0, s, b, anchor[:, s * lanes : (s + 1) * lanes])

    def rows_of(q, r):
        return pl.ds(pl.multiple_of(r * halves[q], 8), halves[q])

    def near(p, s, q):
        ref = tables[p][s][q].at[pl.ds(col * blocks_dev, blocks_dev)]
        return pltpu.make_async_remote_copy(
            src_ref=ref, dst_ref=ref,
            send_sem=near_send.at[p, s, q], recv_sem=near_recv.at[p, s, q],
            device_id=(row, mate), device_id_type=MESH,
        )

    def far(p, s, j, q, d):
        r = (low + d) % 2
        ref = tables[p][s][q].at[pl.ds(col * blocks_dev, blocks_dev), rows_of(q, r), :]
        return pltpu.make_async_remote_copy(
            src_ref=ref, dst_ref=ref,
            send_sem=far_send.at[p, s, j - 1, q, d], recv_sem=far_recv.at[p, s, j - 1, q, d],
            device_id=(row, ((pair + j) % pairs) * 2 + r), device_id_type=MESH,
        )

    def forward(p, s, j, q):
        first = ((pair + pairs - j) % pairs) * 2 * blocks_dev
        return pltpu.make_async_remote_copy(
            src_ref=tables[p][s][q].at[pl.ds(first, 2 * blocks_dev), rows_of(q, low), :],
            dst_ref=landed[p][s][q].at[pl.ds((j - 1) * 2 * blocks_dev, 2 * blocks_dev)],
            send_sem=fwd_send.at[p, s, j - 1, q], recv_sem=fwd_recv.at[p, s, j - 1, q],
            device_id=(row, mate), device_id_type=MESH,
        )

    def sums_near(p):
        ref = sums[p].at[pl.ds(col * blocks_dev, blocks_dev)]
        return pltpu.make_async_remote_copy(
            src_ref=ref, dst_ref=ref, send_sem=sums_send.at[p, 0], recv_sem=sums_recv.at[p, 0],
            device_id=(row, mate), device_id_type=MESH,
        )

    def sums_far(p, j, d):
        ref = sums[p].at[pl.ds(col * blocks_dev, blocks_dev)]
        return pltpu.make_async_remote_copy(
            src_ref=ref, dst_ref=ref,
            send_sem=sums_send.at[p, j], recv_sem=sums_recv.at[p, 2 * j - 1 + d],
            device_id=(row, ((pair + j) % pairs) * 2 + 1), device_id_type=MESH,
        )

    def sums_forward(p, j):
        first = ((pair + pairs - j) % pairs) * 2 * blocks_dev
        ref = sums[p].at[pl.ds(first, 2 * blocks_dev)]
        return pltpu.make_async_remote_copy(
            src_ref=ref, dst_ref=ref,
            send_sem=sums_send.at[p, pairs - 1 + j], recv_sem=sums_recv.at[p, 2 * (pairs - 1) + j],
            device_id=(row, mate), device_id_type=MESH,
        )

    def start_sums(p):
        for j in range(1, pairs):
            sums_far(p, j, low).start()
        sums_near(p).start()

    def start_gather(p, s, q):
        for j in range(1, pairs):
            for d in range(2):
                far(p, s, j, q, d).start()
        near(p, s, q).start()

    def relay_sums(p):
        sums_near(p).wait_recv()

        @pl.when(low == 1)
        def _():
            for j in range(1, pairs):
                for d in range(2):
                    sums_far(p, j, d).wait_recv()

            def answer(other):
                for r in range(2):
                    sums_reply[r, other] = sums[p][asked_s[r, other, 0, row]]
                    pltpu.make_async_remote_copy(
                        src_ref=sums_reply.at[r, other], dst_ref=sums_remote.at[p, row],
                        send_sem=srep_send.at[p], recv_sem=srep_recv.at[p],
                        device_id=(other, pair * 2 + r), device_id_type=MESH,
                    ).start()

            each_peer(answer)
            for j in range(1, pairs):
                sums_forward(p, j).start()

    def relay(p, s, steps):
        for kind, q in [(text[0], int(text[1:] or 0)) for text in steps]:
            if kind == "G":
                start_gather(p, s, q)
                continue
            if kind == "S":
                sum_rows(p, s)
                if s == STREAMS - 1:
                    start_sums(p)
                continue
            if kind == "U":
                if s == STREAMS - 1:
                    relay_sums(p)
                continue
            for j in range(1, pairs):
                for d in range(2):
                    far(p, s, j, q, d).wait_recv()
            near(p, s, q).wait_recv()
            rows_q = pl.ds(pl.multiple_of(starts[q] + low * halves[q], 8), halves[q])

            def answer(other):
                for r in range(2):
                    reply[s, r, other, rows_q, :] = tables[p][s][q][
                        asked_s[r, other, 0, row], rows_of(q, low), :
                    ]
                    pltpu.make_async_remote_copy(
                        src_ref=reply.at[s, r, other, rows_q, :],
                        dst_ref=remote.at[p, s, row, rows_q, :],
                        send_sem=rep_send.at[p, s], recv_sem=rep_recv.at[p, s, q],
                        device_id=(other, pair * 2 + r), device_id_type=MESH,
                    ).start()

            each_peer(answer)
            for j in range(1, pairs):
                forward(p, s, j, q).start()

    def product(p, s, b, q):
        rhs = [tables[p][s][q][index_ref[b * degree + k]] for k in range(degree)]
        return jnp.dot(
            adj_q[q][b], jnp.concatenate(rhs, axis=0), preferred_element_type=jnp.float32
        )

    def row_scale(p, b):
        here = slice(b * block_rows, (b + 1) * block_rows)
        total = jnp.zeros((block_rows, block_rows), jnp.float32)
        for k in range(degree):
            total = total + adj[b, k].astype(jnp.float32) * sums[p][index_ref[b * degree + k]]
        rest = anchor_ref[here, :block_rows]
        for i in range(1, classes // block_rows):
            rest = rest + anchor_ref[here, i * block_rows : (i + 1) * block_rows]
        total = ALPHA * total + (1.0 - ALPHA) * rest
        return classes / jnp.sum(total, axis=1, keepdims=True)

    def blend(p, s, b, q, mine):
        here = slice(b * block_rows, (b + 1) * block_rows)
        spread = product(p, s, b, q)
        if q > 0:
            spread = spread + blend_ref[s, here, :]
        if q < CHUNKS - 1:
            return spread
        return ALPHA * spread + (1.0 - ALPHA) * anchor_ref[here, mine]

    blended = {}

    def gathered(p, s, q):
        rows_q = pl.ds(starts[q], sizes[q])
        got = remote.at[p, s, pl.ds(0, peers), rows_q, :]
        pltpu.make_async_copy(got, got, rep_recv.at[p, s, q]).wait()
        for j in range(1, pairs):
            forward(p, s, j, q).wait_recv()
            first = ((pair + pairs - j) % pairs) * 2 * blocks_dev
            tables[p][s][q][pl.ds(first, 2 * blocks_dev), rows_of(q, 1 - low), :] = landed[p][s][q][
                pl.ds((j - 1) * 2 * blocks_dev, 2 * blocks_dev)
            ]

        def fold(other):
            tables[p][s][q][group + other] = remote[p, s, other, rows_q, :]

        each_peer(fold)

    def partial(h, s, q):
        p = h % 2
        gathered(p, s, q)
        for b in range(blocks_dev):
            here = slice(b * block_rows, (b + 1) * block_rows)
            blend_ref[s, here, :] = blend(p, s, b, q, slice(s * lanes, (s + 1) * lanes))
        blended[h, s] = q + 1

    def finish(h, s):
        p, last = h % 2, h == HOPS - 1
        mine = slice(s * lanes, (s + 1) * lanes)
        for q in range(blended.get((h, s), 0), CHUNKS - (s > 0)):
            partial(h, s, q)
        if s > 0:
            gathered(p, s, CHUNKS - 1)

        if s == 0:
            got = sums_remote.at[p, pl.ds(0, peers)]
            pltpu.make_async_copy(got, got, srep_recv.at[p]).wait()

            @pl.when(low == 0)
            def _():
                for j in range(1, pairs):
                    sums_forward(p, j).wait_recv()

            def fold_sums(other):
                sums[p][group + other] = sums_remote[p, other]

            each_peer(fold_sums)

        for b in range(blocks_dev):
            here = slice(b * block_rows, (b + 1) * block_rows)
            if s == 0:
                scale = jnp.broadcast_to(row_scale(p, b), (block_rows, lanes))
                scale_ref[here, :] = scale
                labels = blend_ref[s, here, :] * scale
            else:
                labels = blend(p, s, b, CHUNKS - 1, mine) * scale_ref[here, :]
            if last:
                out_ref[here, mine] = labels
            else:
                keep(1 - p, s, b, labels)

        for q in range(CHUNKS):
            for j in range(1, pairs):
                for d in range(2):
                    far(p, s, j, q, d).wait_send()
                forward(p, s, j, q).wait_send()
            near(p, s, q).wait_send()
        for r in range(2):
            sent = reply.at[s, r, pl.ds(0, peers), pl.ds(0, block_rows // 2), :]
            pltpu.make_async_copy(sent, sent, rep_send.at[p, s]).wait()
        if s == STREAMS - 1:
            for j in range(1, pairs):
                sums_far(p, j, low).wait_send()
            sums_near(p).wait_send()

            @pl.when(low == 1)
            def _():
                sent = sums_reply.at[:, pl.ds(0, peers)]
                pltpu.make_async_copy(sent, sent, srep_send.at[p]).wait()
                for j in range(1, pairs):
                    sums_forward(p, j).wait_send()


    for s in range(STREAMS):
        relay(0, s, ["S"])
    for s in range(STREAMS):
        relay(0, s, HEAD)

    all_asked = asked_v.at[:, pl.ds(0, peers)]
    pltpu.make_async_copy(all_asked, all_asked, asked_recv).wait()
    pltpu.make_async_copy(all_asked, all_asked, asked_send).wait()
    to_scalar = pltpu.make_async_copy(asked_v, asked_s, asked_copy)
    to_scalar.start()
    to_scalar.wait()

    relay_sums(0)
    for s in range(STREAMS):
        relay(0, s, EARLY)
        if s < STREAMS - 1:
            relay(0, s, LATE)
    adj_copy.wait()
    for b in range(blocks_dev):
        for q in range(CHUNKS):
            columns = slice(starts[q], starts[q] + sizes[q])
            adj_q[q][b] = jnp.concatenate([adj[b, k][:, columns] for k in range(degree)], axis=1)
    left = (0, STREAMS - 1)

    for h in range(HOPS):
        p = (h + 1) % 2
        for s in range(STREAMS):
            finish(h, s)
            if h < HOPS - 1:
                relay(p, s, ["S"] + HEAD if s == STREAMS - 1 else HEAD + ["S"])
            if left is not None:
                relay(*left, LATE)
                left = None
            if h < HOPS - 1:
                pending = (h, s + 1) if s < STREAMS - 1 else (h + 1, 0)
                for text in BETWEEN[s > 0]:
                    if text[0] == "M":
                        partial(*pending, int(text[1:]))
                    else:
                        relay(p, s, [text])
                left = (p, s)
                if h == HOPS - 2 and s == STREAMS - 1:
                    relay(p, s, LATE)
                    left = None


def local(adjacency_tiles, col_block, label_prior, seed_label, seed_mask):
    blocks_dev, degree, block_rows, _ = adjacency_tiles.shape
    nodes, classes = label_prior.shape
    n_rows = lax.axis_size("rows")
    n_cols = lax.axis_size("cols")
    group = n_cols * blocks_dev
    lanes = classes // STREAMS
    padded = -(-n_rows // LANES) * LANES
    pairs = max(n_cols // 2, 2)
    span = (pairs - 1) * 2 * blocks_dev
    unit = block_rows // sum(CHUNK_PARTS)
    dma = pltpu.SemaphoreType.DMA
    vmem = pl.BlockSpec(memory_space=pltpu.VMEM)
    return pl.pallas_call(
        functools.partial(kernel, n_rows, n_cols, blocks_dev, degree, block_rows, classes),
        out_shape=jax.ShapeDtypeStruct((nodes, classes), jnp.float32),
        in_specs=[
            pl.BlockSpec(memory_space=pl.ANY),
        ] * 5,
        out_specs=vmem,
        scratch_shapes=[
            [
                [
                    [
                        pltpu.VMEM((group + n_rows, unit * part, lanes), jnp.bfloat16)
                        for part in CHUNK_PARTS
                    ]
                    for _ in range(STREAMS)
                ]
                for _ in range(2)
            ],
            pltpu.VMEM((2, STREAMS, n_rows, block_rows, lanes), jnp.bfloat16),
            pltpu.VMEM((STREAMS, 2, n_rows, block_rows, lanes), jnp.bfloat16),
            [
                [
                    [pltpu.VMEM((span, unit * part // 2, lanes), jnp.bfloat16) for part in CHUNK_PARTS]
                    for _ in range(STREAMS)
                ]
                for _ in range(2)
            ],
            [pltpu.VMEM((group + n_rows, 1, block_rows), jnp.float32) for _ in range(2)],
            pltpu.VMEM((2, n_rows, 1, block_rows), jnp.float32),
            pltpu.VMEM((2, n_rows, 1, block_rows), jnp.float32),
            pltpu.VMEM((blocks_dev, 1, block_rows), jnp.float32),
            pltpu.VMEM((nodes, lanes), jnp.float32),
            pltpu.VMEM((STREAMS, nodes, lanes), jnp.float32),
            [
                pltpu.VMEM((blocks_dev, block_rows, degree * unit * part), jnp.bfloat16)
                for part in CHUNK_PARTS
            ],
            pltpu.VMEM(adjacency_tiles.shape, jnp.bfloat16),
            pltpu.VMEM((nodes, classes), jnp.float32),
            pltpu.SMEM((blocks_dev * degree,), jnp.int32),
            pltpu.VMEM((1, padded), jnp.int32),
            pltpu.VMEM((2, n_rows, 1, padded), jnp.int32),
            pltpu.SMEM((2, n_rows, 1, padded), jnp.int32),
            pltpu.SMEM(col_block.shape, jnp.int32),
            pltpu.VMEM((nodes, classes), jnp.float32),
            pltpu.VMEM((blocks_dev, block_rows), jnp.int32),
            pltpu.VMEM((blocks_dev, block_rows), jnp.int32),
            dma((4,)),
            dma, dma, dma, dma,
            dma((2, STREAMS, CHUNKS)), dma((2, STREAMS, CHUNKS)),
            dma((2, STREAMS, pairs - 1, CHUNKS, 2)), dma((2, STREAMS, pairs - 1, CHUNKS, 2)),
            dma((2, STREAMS, pairs - 1, CHUNKS)), dma((2, STREAMS, pairs - 1, CHUNKS)),
            dma((2, STREAMS)), dma((2, STREAMS, CHUNKS)),
            dma((2, 2 * pairs - 1)), dma((2, 3 * pairs - 2)),
            dma((2,)), dma((2,)),
        ],
        compiler_params=pltpu.CompilerParams(
            collective_id=0, has_side_effects=True, vmem_limit_bytes=VMEM_LIMIT - 4 * nodes * classes - SPARE
        ),
    )(
        col_block,
        label_prior,
        seed_label.reshape(blocks_dev, block_rows),
        seed_mask.reshape(blocks_dev, block_rows),
        adjacency_tiles,
    )


def solution(mesh):
    in_specs = (
        P(("rows", "cols"), None, None, None),
        P(("rows", "cols"), None),
        P(("rows", "cols"), None),
        P(("rows", "cols")),
        P(("rows", "cols")),
    )
    out_specs = P(("rows", "cols"), None)
    return jax.shard_map(local, mesh=mesh, in_specs=in_specs, out_specs=out_specs, check_vma=False)
```
